32 devices in a mesh: dp: 4 (over x, y), tp: 8 (over z, core).
Axes of the slice: x: 2, y: 2, z: 4, core: 2. Of those that a mesh axis runs over, the one named last changes fastest.
Arguments:
- x: bfloat16 [4096, 8192], P(('dp', 'tp')), parts along dimension 0
- gain: bfloat16 [8192], replicated
- wq: bfloat16 [8192, 8192], P(None, 'tp')
- wk: bfloat16 [8192, 8192], P(None, 'tp')
- wv: bfloat16 [8192, 8192], P(None, 'tp')
- wo: bfloat16 [8192, 8192], P('tp')
Outputs:
- output: bfloat16 [4096, 8192], P(('dp', 'tp')), parts along dimension 0
There are 4 independent parts. The reference program is written for one: setup_inputs(seed, part) draws one part's arguments, and reference() takes and returns one part's arrays. A program takes and returns all parts, laid end to end along the dimension named above; an argument that names none is the same for every part.
All inputs are finite; a program needn't handle non-finite values.
Results may differ from the reference program's by a relative error of at most 0.012.
Values are sent between devices in bfloat16 or wider.
A program may use at most 2 GiB of HBM per device.

```python
import jax
import jax.numpy as jnp
from jax import lax

ROWS = 1024
D = 8192
HEADS = 64
KV_HEADS = 64
HEAD = 128
THETA = 10000


def setup_inputs(seed: int = 0, part: int = 0) -> dict:
    kx, kn, kq, kk, kv, ko = jax.random.split(jax.random.key(seed), 6)

    def weights(key, rows, columns):
        return jax.random.normal(key, (rows, columns), jnp.float32) * rows**-0.5

    drawn = {
        "x": jax.random.normal(jax.random.fold_in(kx, part), (ROWS, D), jnp.float32),
        "gain": 1 + 0.1 * jax.random.normal(kn, (D,), jnp.float32),
        "wq": 2 * weights(kq, D, HEADS * HEAD),
        "wk": 2 * weights(kk, D, KV_HEADS * HEAD),
        "wv": 4 * weights(kv, D, KV_HEADS * HEAD),
        "wo": weights(ko, HEADS * HEAD, D),
    }
    return {k: v.astype(jnp.bfloat16) for k, v in drawn.items()}


def normed(x, gain):
    wide = x.astype(jnp.float32)
    scale = lax.rsqrt(jnp.mean(wide * wide, -1, keepdims=True) + 1e-6)
    return (wide * scale * gain.astype(jnp.float32)).astype(jnp.bfloat16)


def turned(t, place, theta):
    half = t.shape[-1] // 2
    angle = place.astype(jnp.float32)[:, None] * theta ** (-jnp.arange(half, dtype=jnp.float32) / half)
    cos, sin = jnp.cos(angle)[:, None], jnp.sin(angle)[:, None]
    a, b = t[..., :half].astype(jnp.float32), t[..., half:].astype(jnp.float32)
    return jnp.concatenate([a * cos - b * sin, b * cos + a * sin], -1).astype(jnp.bfloat16)


def matmul(a, w):
    return jnp.dot(a, w, preferred_element_type=jnp.float32).astype(jnp.bfloat16)


def einsum(form, a, b):
    return jnp.einsum(form, a.astype(jnp.float32), b.astype(jnp.float32))


def attention(q, k, v):
    scores = einsum("tgsd,ugd->gstu", q, k) * q.shape[-1] ** -0.5
    token = jnp.arange(q.shape[0])
    scores = jnp.where(token[:, None] >= token, scores, -jnp.inf)
    weights = jax.nn.softmax(scores, -1).astype(jnp.bfloat16)
    return einsum("gstu,ugd->tgsd", weights, v).astype(jnp.bfloat16)


def reference(x, gain, wq, wk, wv, wo):
    a, place = normed(x, gain), jnp.arange(ROWS)
    q = turned(matmul(a, wq).reshape(ROWS, HEADS, HEAD), place, THETA).reshape(ROWS, KV_HEADS, -1, HEAD)
    k = turned(matmul(a, wk).reshape(ROWS, KV_HEADS, HEAD), place, THETA)
    v = matmul(a, wv).reshape(ROWS, KV_HEADS, HEAD)
    seen = attention(q, k, v).reshape(ROWS, HEADS * HEAD)
    return (x.astype(jnp.float32) + jnp.dot(seen, wo, preferred_element_type=jnp.float32)).astype(jnp.bfloat16)
```

```python
import functools

import jax
import jax.numpy as jnp
from jax import lax
from jax.experimental import pallas as pl
from jax.experimental.pallas import tpu as pltpu
from jax.sharding import PartitionSpec as P

HEAD = 128
THETA = 10000
NB = 8
HIDDEN = -2e30
LOG2E = 1.4426950408889634
MESH = pl.DeviceIdType.MESH
F32, BF16 = jnp.float32, jnp.bfloat16


def _dot(a, b, ca=1, cb=0):
    return lax.dot_general(a, b, (((ca,), (cb,)), ((), ())), preferred_element_type=F32)


def _kernel(a_ref, wq_ref, wk_ref, wv_ref, wo_ref, rope_ref, y_ref,
            xg, wbuf, wob, acc, q_s, k_s, vt_s, mix_s, top_s, second, term, pst, nst, fst,
            own_m, w_m, wo_m, up_m, dn_m, pa_m, nb_r, pa_r, tp_m, tp_r, ns_m, nr_r, sec_r, y_m, pcred, ncred):
    RB, D = a_ref.shape
    HD = wq_ref.shape[1]
    H = HD // HEAD
    KB = D // NB
    C = 2 * RB
    TN = min(512, HD)
    me = lax.axis_index("tp")
    z, r = me // 2, me % 2
    up, dn, partner = {"tp": me + 2}, {"tp": me - 2}, {"tp": me + 1 - 2 * r}
    weights = (wq_ref, wk_ref, wv_ref)

    def remote(src, dst, send, recv, to):
        return pltpu.make_async_remote_copy(src_ref=src, dst_ref=dst, send_sem=send, recv_sem=recv, device_id=to, device_id_type=MESH)

    def mine(k):
        return a_ref.at[:, pl.ds(pl.multiple_of(k * KB, KB), KB)]

    def half(c, k, h):
        return xg.at[c, k, pl.ds(pl.multiple_of(h * RB, RB), RB), :]

    def gather_up(c, k, src):
        return remote(src, half(c, k, r), up_m.at[c, k], nb_r.at[c, k], up)

    def gather_dn(c, k, src):
        return remote(src, half(c, k, r), dn_m.at[c, k], nb_r.at[c, k], dn)

    def gather_pa(c, k, src):
        return remote(src, half(c, k, r), pa_m.at[c, k], pa_r.at[c, k], partner)

    def got_pa(c, k):
        remote(half(c, k, 1 - r), half(c, k, 1 - r), pa_m.at[c, k], pa_r.at[c, k], partner).wait_recv()

    def own_copy(k):
        return pltpu.make_async_copy(mine(k), half(z, k, r), own_m.at[k])

    def w_copies(g):
        at = pl.ds(pl.multiple_of((g % NB) * KB, KB), KB)
        return [pltpu.make_async_copy(weights[i].at[at, :], wbuf.at[g % 2, i], w_m.at[g % 2, i]) for i in range(3)]

    def wo_copy(j):
        return pltpu.make_async_copy(wo_ref.at[:, pl.ds(pl.multiple_of(j * KB, KB), KB)], wob.at[j % 3], wo_m.at[j % 3])

    def loop(n, body):
        lax.fori_loop(0, n, lambda i, _: body(i), None)

    def comm(s, k):
        @pl.when(z > s)
        def _():
            gather_up(s, k, half(s, k, r)).wait_recv()

            @pl.when(z < 3)
            def _():
                gather_up(s, k, half(s, k, r)).start()

            gather_pa(s, k, half(s, k, r)).start()

        d = z + 1 + s

        @pl.when(d <= 3)
        def _():
            gather_dn(d, k, half(d, k, r)).wait_recv()

            @pl.when(z > 0)
            def _():
                gather_dn(d, k, half(d, k, r)).start()

            gather_pa(d, k, half(d, k, r)).start()

    def freed(c):
        @pl.when((z > c) & (z < 3))
        def _():
            loop(NB, lambda k: gather_up(c, k, half(c, k, r)).wait_send())

        @pl.when((z < c) & (z > 0))
        def _():
            loop(NB, lambda k: gather_dn(c, k, half(c, k, r)).wait_send())

        loop(NB, lambda k: gather_pa(c, k, half(c, k, r)).wait_send())
        pl.semaphore_signal(pcred.at[c], 1, device_id=partner, device_id_type=MESH)

        @pl.when((c <= z) & (z < 3))
        def _():
            pl.semaphore_signal(ncred.at[c], 1, device_id=up, device_id_type=MESH)

        @pl.when((c >= z) & (z > 0))
        def _():
            pl.semaphore_signal(ncred.at[c], 1, device_id=dn, device_id_type=MESH)

    def project(g, k, chunks):
        n = HD // TN

        def tile(t):
            i, at = t // n, pl.multiple_of((t % n) * TN, TN)
            w = wbuf[g % 2, i, :, pl.ds(at, TN)]
            cols = pl.ds(pl.multiple_of(t * TN, TN), TN)
            for p, c in enumerate(chunks):
                acc[p, :, cols] += _dot(xg[c, k], w)

        loop(3 * n, tile)

    def turn(p, c):
        rows = pl.ds(pl.multiple_of(c * C, C), C)
        cos, sin = rope_ref[0, rows, :], rope_ref[1, rows, :]

        def turned(t):
            t = t.astype(BF16).astype(F32)
            return (t * cos + pltpu.roll(t, HEAD // 2, 1) * sin).astype(BF16)

        for h in range(H):
            at = h * HEAD
            q_s[c, :, at : at + HEAD] = turned(acc[p, :, at : at + HEAD])
            k_s[c, h] = turned(acc[p, :, HD + at : HD + at + HEAD])
            vt_s[c, h] = acc[p, :, 2 * HD + at : 2 * HD + at + HEAD].astype(BF16).T

    def attend(c):
        e = HEAD**-0.5 * LOG2E
        ones = jnp.ones((8, C), BF16)

        def scores(kb):
            return [_dot(k_s[kb, h], q_s[c, :, h * HEAD : (h + 1) * HEAD], 1, 1) for h in range(H)]

        def values(kb, h):
            return jnp.concatenate([vt_s[kb, h], ones], axis=0)

        ok = lax.broadcasted_iota(jnp.int32, (C, C), 1) >= lax.broadcasted_iota(jnp.int32, (C, C), 0)
        for h, s in enumerate(scores(c)):
            s = jnp.where(ok, s, HIDDEN)
            top = s.max(axis=0, keepdims=True)
            top_s[h : h + 1, :] = top
            mix_s[h] = _dot(values(c, h), jnp.exp2((s - top) * e).astype(BF16))

        def block(kb, _):
            weights, keeps = [], []
            for h, s in enumerate(scores(kb)):
                old = top_s[h : h + 1, :]
                top = jnp.maximum(old, s.max(axis=0, keepdims=True))
                top_s[h : h + 1, :] = top
                weights.append(jnp.exp2((s - top) * e).astype(BF16))
                keeps.append(jnp.exp2((old - top) * e))
            for h in range(H):
                mix_s[h] = mix_s[h] * keeps[h] + _dot(values(kb, h), weights[h])

        lax.fori_loop(0, c, block, None)
        for h in range(H):
            out = mix_s[h, :HEAD, :] * (1 / mix_s[h, HEAD : HEAD + 1, :])
            q_s[c, :, h * HEAD : (h + 1) * HEAD] = out.T.astype(BF16)

    def my_rows(w, j):
        return term.at[w, j % 2, pl.ds(pl.multiple_of(r * RB, RB), RB), :]

    def to_partner(w, c, j):
        return remote(pst.at[w, j % 2], xg.at[c, j, pl.ds(RB, RB), :], tp_m.at[w, j % 2], tp_r.at[c, j], partner)

    def run_dn(c, j):
        return remote(nst.at[j], xg.at[c, j, pl.ds(0, RB), :], ns_m.at[j], nr_r.at[c, j], dn)

    def run_up(c, j):
        return remote(nst.at[j], xg.at[c, j, pl.ds(0, RB), :], ns_m.at[j], nr_r.at[c, j], up)

    def run_home(j):
        return remote(nst.at[j], second.at[j], ns_m.at[j], sec_r.at[j], up)

    def y_copy(j):
        return pltpu.make_async_copy(fst.at[j], y_ref.at[:, pl.ds(pl.multiple_of(j * KB, KB), KB)], y_m.at[j])

    def wo_start():
        wo_copy(0).start()
        wo_copy(1).start()

    def wo_next(j):
        @pl.when(j + 2 < NB)
        def _():
            wo_copy(j + 2).start()

        wo_copy(j).wait()

    def stage_a(w, c, j):
        @pl.when(j == 0)
        def _():
            pl.semaphore_wait(pcred.at[c], 1)

        tk = min(512, KB)

        def tile(n):
            cols = pl.ds(pl.multiple_of(n * tk, tk), tk)
            term[w, j % 2, :, cols] = _dot(q_s[c], wob[j % 3, :, cols])

        loop(KB // tk, tile)
        theirs = pl.ds(pl.multiple_of((1 - r) * RB, RB), RB)
        pst[w, j % 2] = term[w, j % 2, theirs, :].astype(BF16)
        to_partner(w, c, j).start()

    def stage_b(w, c, j, prior):
        to_partner(w, c, j).wait()
        t = my_rows(w, j)
        t[...] += xg[c, j, RB:, :].astype(F32)

        @pl.when(((c <= z) & (z < 3)) | ((c > z) & (z > 0)))
        def _():
            run_dn(c, j).wait_recv()
            t[...] += xg[c, j, :RB, :].astype(F32)

        if prior is None:
            @pl.when(z > 0)
            def _():
                run_home(j).wait_recv()
                t[...] += second[j].astype(F32)

            fst[j] = t[...].astype(BF16)
            y_copy(j).start()
            return

        @pl.when(prior)
        def _():
            run_dn(c, j).wait_send()

        @pl.when(j == 0)
        def _():
            pl.semaphore_wait(ncred.at[c], 1)

        nst[j] = t[...].astype(BF16)

        @pl.when(c < z)
        def _():
            run_dn(c, j).start()

        @pl.when(c == z + 1)
        def _():
            run_home(j).start()

        @pl.when(c > z + 1)
        def _():
            run_up(c, j).start()

    def stages(j, w, c, prior):
        @pl.when(j < NB)
        def _():
            stage_a(w, c, j)

        @pl.when(j > 0)
        def _():
            stage_b(w, c, j - 1, prior)

    for copy in w_copies(0):
        copy.start()
    loop(NB, lambda k: own_copy(k).start())
    barrier = pltpu.get_barrier_semaphore()
    pl.semaphore_signal(barrier, 1, device_id=partner, device_id_type=MESH)

    @pl.when(z > 0)
    def _():
        pl.semaphore_signal(barrier, 1, device_id=dn, device_id_type=MESH)

    @pl.when(z < 3)
    def _():
        pl.semaphore_signal(barrier, 1, device_id=up, device_id_type=MESH)

    @pl.when((z > 0) & (z < 3))
    def _():
        pl.semaphore_wait(barrier, 3)

    @pl.when((z == 0) | (z == 3))
    def _():
        pl.semaphore_wait(barrier, 2)

    def first_sends(k):
        @pl.when(z == 0)
        def _():
            gather_up(z, k, mine(k)).start()

        @pl.when(z > 0)
        def _():
            gather_dn(z, k, mine(k)).start()

        gather_pa(z, k, mine(k)).start()

    loop(NB, first_sends)
    acc[...] = jnp.zeros_like(acc)

    c0 = (3 - z) // 3

    def slot0(k):
        for copy in w_copies(k + 1):
            copy.start()
        comm(0, k)
        own_copy(k).wait()
        got_pa(z, k)
        got_pa(c0, k)
        for copy in w_copies(k):
            copy.wait()
        project(k, k, (z, c0))

    loop(NB, slot0)

    def later_sends(s):
        @pl.when(z == s)
        def _():
            loop(NB, lambda k: gather_up(z, k, mine(k)).start())

    later_sends(1)
    turn(0, z)
    turn(1, c0)
    freed(c0)

    pl.semaphore_signal(pcred.at[z], 1, device_id=partner, device_id_type=MESH)

    @pl.when(z < 3)
    def _():
        pl.semaphore_signal(ncred.at[z], 1, device_id=up, device_id_type=MESH)

    @pl.when(z > 0)
    def _():
        pl.semaphore_signal(ncred.at[z], 1, device_id=dn, device_id_type=MESH)

    firsts = (0, 2 - z // 2, 3 - z // 3, 4)
    lax.fori_loop(firsts[0], firsts[1], lambda c, _: attend(c), None)

    for s in (1, 2):
        cp = (2 - z // 2, 3 - z // 3)[s - 1]
        cs = (1 - z // 3, 2 - 2 * (z // 2) + z // 3)[s - 1]
        summing = ((z == 0) | (z == 3)) if s == 1 else (z >= 0)
        prior = (z < 0) if s == 1 else ((z == 0) | (z == 3))
        acc[0] = jnp.zeros_like(acc[0])

        @pl.when(summing)
        def _():
            wo_start()

        def slot(k):
            g = s * NB + k

            @pl.when(k < NB)
            def _():
                @pl.when(g + 1 < 3 * NB)
                def _():
                    for copy in w_copies(g + 1):
                        copy.start()

                comm(s, k)
                got_pa(cp, k)
                for copy in w_copies(g):
                    copy.wait()
                project(g, k, (cp,))

            @pl.when(summing)
            def _():
                @pl.when(k < NB)
                def _():
                    wo_next(k)

                stages(k, 0, cs, prior)

        loop(NB + 1, slot)
        if s == 1:
            later_sends(2)
        else:
            wo_start()
        turn(0, cp)
        freed(cp)
        lax.fori_loop(firsts[s], firsts[s + 1], lambda c, _: attend(c), None)

    def last(j):
        @pl.when(j < NB)
        def _():
            wo_next(j)

        stages(j, 0, (z + 3) % 4, z >= 0)

    loop(NB + 1, last)
    wo_start()

    def home(j):
        @pl.when(j < NB)
        def _():
            wo_next(j)

        @pl.when((z == 1) | (z == 2))
        def _():
            stages(j, 0, 3, z >= 0)

        stages(j, 1, z, None)

    loop(NB + 1, home)

    def rest(k):
        y_copy(k).wait()
        run_dn(0, k).wait_send()
        gather_pa(z, k, mine(k)).wait_send()

        @pl.when(z > 0)
        def _():
            gather_dn(z, k, mine(k)).wait_send()

        @pl.when(z < 3)
        def _():
            gather_up(z, k, mine(k)).wait_send()

    loop(NB, rest)


def _fused(a, wq, wk, wv, wo, rope):
    RB, D = a.shape
    HD = wq.shape[1]
    H, KB, C = HD // HEAD, D // NB, 2 * RB
    dma = pltpu.SemaphoreType.DMA
    return pl.pallas_call(
        _kernel,
        out_shape=jax.ShapeDtypeStruct((RB, D), BF16),
        in_specs=[pl.BlockSpec(memory_space=pl.ANY)] * 5 + [pl.BlockSpec(memory_space=pltpu.VMEM)],
        out_specs=pl.BlockSpec(memory_space=pl.ANY),
        scratch_shapes=[
            pltpu.VMEM((4, NB, C, KB), BF16),
            pltpu.VMEM((2, 3, KB, HD), BF16),
            pltpu.VMEM((3, HD, KB), BF16),
            pltpu.VMEM((2, C, 3 * HD), F32),
            pltpu.VMEM((4, C, HD), BF16),
            pltpu.VMEM((4, H, C, HEAD), BF16),
            pltpu.VMEM((4, H, HEAD, C), BF16),
            pltpu.VMEM((H, HEAD + 8, C), F32),
            pltpu.VMEM((H, C), F32),
            pltpu.VMEM((NB, RB, KB), BF16),
            pltpu.VMEM((2, 2, C, KB), F32),
            pltpu.VMEM((2, 2, RB, KB), BF16),
            pltpu.VMEM((NB, RB, KB), BF16),
            pltpu.VMEM((NB, RB, KB), BF16),
            dma((NB,)),
            dma((2, 3)),
            dma((3,)),
            dma((4, NB)),
            dma((4, NB)),
            dma((4, NB)),
            dma((4, NB)),
            dma((4, NB)),
            dma((2, 2)),
            dma((4, NB)),
            dma((NB,)),
            dma((4, NB)),
            dma((NB,)),
            dma((NB,)),
            pltpu.SemaphoreType.REGULAR((4,)),
            pltpu.SemaphoreType.REGULAR((4,)),
        ],
        compiler_params=pltpu.CompilerParams(collective_id=0, has_side_effects=True, vmem_limit_bytes=67043328),
    )(a, wq, wk, wv, wo, rope)


def normed(x, gain):
    wide = x.astype(F32)
    scale = lax.rsqrt(jnp.mean(wide * wide, -1, keepdims=True) + 1e-6)
    return (wide * scale * gain.astype(F32)).astype(BF16)


def solution(mesh):
    def step(x, gain, wq, wk, wv, wo):
        rows = x.shape[0] * mesh.shape["tp"]
        half = HEAD // 2
        angle = jnp.arange(rows).astype(F32)[:, None] * THETA ** (-jnp.arange(half, dtype=F32) / half)
        cos, sin = jnp.cos(angle), jnp.sin(angle)
        rope = jnp.stack([jnp.concatenate([cos, cos], 1), jnp.concatenate([-sin, sin], 1)])
        total = _fused(normed(x, gain), wq, wk, wv, wo, rope)
        return (x.astype(F32) + total.astype(F32)).astype(BF16)

    tokens, columns = P(("dp", "tp"), None), P(None, "tp")
    return jax.shard_map(
        step,
        mesh=mesh,
        in_specs=(tokens, P(None), columns, columns, columns, P("tp", None)),
        out_specs=tokens,
        check_vma=False,
    )
```

```python
import jax
import jax.numpy as jnp
import numpy as np
from jax import lax
from jax.experimental import pallas as pl
from jax.experimental.pallas import tpu as pltpu
from jax.sharding import PartitionSpec as P

HEAD = 128
THETA = 10000
NB = 16
HIDDEN = -2e30
LOG2E = 1.4426950408889634
LAGS = (6, 5, 0)
MESH = pl.DeviceIdType.MESH
F32, BF16 = jnp.float32, jnp.bfloat16


def _dot(a, b, ca=1, cb=0):
    return lax.dot_general(a, b, (((ca,), (cb,)), ((), ())), preferred_element_type=F32)


def _kernel(x_ref, gain_ref, wq_ref, wk_ref, wv_ref, wo_ref, rope_ref, y_ref,
            xv, an, rope, xg, wbuf, wob, acc, q_s, k_s, vt_s, mix_s, top_s, second, term, pst, nst,
            x_m, rope_m, w_m, wo_m, up_m, dn_m, pa_m, nb_r, pa_r, tp_m, tp_r, ns_m, nr_r, sec_r, y_m, pcred, ncred):
    RB, D = x_ref.shape
    HD = wq_ref.shape[1]
    H = HD // HEAD
    KB = D // NB
    C = 2 * RB
    TN = HD
    me = lax.axis_index("tp")
    z, r = me // 2, me % 2
    up, dn, partner = {"tp": me + 2}, {"tp": me - 2}, {"tp": me + 1 - 2 * r}
    weights = (wq_ref, wk_ref, wv_ref)

    def remote(src, dst, send, recv, to):
        return pltpu.make_async_remote_copy(src_ref=src, dst_ref=dst, send_sem=send, recv_sem=recv, device_id=to, device_id_type=MESH)

    def half(c, k, h):
        return xg.at[c, k, pl.ds(pl.multiple_of(h * RB, RB), RB), :]

    def gather_up(c, k, src):
        return remote(src, half(c, k, r), up_m.at[c, k], nb_r.at[c, k], up)

    def gather_dn(c, k, src):
        return remote(src, half(c, k, r), dn_m.at[c, k], nb_r.at[c, k], dn)

    def gather_pa(c, k, src):
        return remote(src, half(c, k, r), pa_m.at[c, k], pa_r.at[c, k], partner)

    def got_pa(c, k):
        remote(half(c, k, 1 - r), half(c, k, 1 - r), pa_m.at[c, k], pa_r.at[c, k], partner).wait_recv()

    def x_copy(k):
        return pltpu.make_async_copy(x_ref.at[:, pl.ds(pl.multiple_of(k * KB, KB), KB)], xv.at[k], x_m.at[k])

    def w_copies(g):
        at = pl.ds(pl.multiple_of((g % NB) * KB, KB), KB)
        return [pltpu.make_async_copy(weights[i].at[at, :], wbuf.at[g % 4, i], w_m.at[g % 4, i]) for i in range(3)]

    def wo_copy(j):
        return pltpu.make_async_copy(wo_ref.at[:, pl.ds(pl.multiple_of(j * KB, KB), KB)], wob.at[j % 3], wo_m.at[j % 3])

    def loop(n, body):
        lax.fori_loop(0, n, lambda i, _: body(i), None)

    def comm(s, k):
        @pl.when(z > s)
        def _():
            gather_up(s, k, half(s, k, r)).wait_recv()

            @pl.when(z < 3)
            def _():
                gather_up(s, k, half(s, k, r)).start()

            gather_pa(s, k, half(s, k, r)).start()

        d = z + 1 + s

        @pl.when(d <= 3)
        def _():
            gather_dn(d, k, half(d, k, r)).wait_recv()

            @pl.when(z > 0)
            def _():
                gather_dn(d, k, half(d, k, r)).start()

            gather_pa(d, k, half(d, k, r)).start()

    def freed(c):
        @pl.when((z > c) & (z < 3))
        def _():
            loop(NB, lambda k: gather_up(c, k, half(c, k, r)).wait_send())

        @pl.when((z < c) & (z > 0))
        def _():
            loop(NB, lambda k: gather_dn(c, k, half(c, k, r)).wait_send())

        loop(NB, lambda k: gather_pa(c, k, half(c, k, r)).wait_send())
        pl.semaphore_signal(pcred.at[c], 1, device_id=partner, device_id_type=MESH)

        @pl.when((c <= z) & (z < 3))
        def _():
            pl.semaphore_signal(ncred.at[c], 1, device_id=up, device_id_type=MESH)

        @pl.when((c >= z) & (z > 0))
        def _():
            pl.semaphore_signal(ncred.at[c], 1, device_id=dn, device_id_type=MESH)

    def project(g, k, chunks):
        n = HD // TN

        def tile(t):
            i, at = t // n, pl.multiple_of((t % n) * TN, TN)
            w = wbuf[g % 4, i, :, pl.ds(at, TN)]
            cols = pl.ds(pl.multiple_of(t * TN, TN), TN)
            for p, c in enumerate(chunks):
                acc[p, :, cols] += _dot(xg[c, k], w)

        loop(3 * n, tile)

    def turn(p, c):
        rows = pl.ds(pl.multiple_of(c * C, C), C)
        cs = rope[rows, :]
        sc = pltpu.roll(cs, HEAD // 2, 1)
        first = lax.broadcasted_iota(jnp.int32, cs.shape, 1) < HEAD // 2
        cos, sin = jnp.where(first, cs, sc), jnp.where(first, -sc, cs)

        def turned(t):
            t = t.astype(BF16).astype(F32)
            return (t * cos + pltpu.roll(t, HEAD // 2, 1) * sin).astype(BF16)

        for h in range(H):
            at = h * HEAD
            q_s[c, :, at : at + HEAD] = turned(acc[p, :, at : at + HEAD])
            k_s[c, h] = turned(acc[p, :, HD + at : HD + at + HEAD])
            vt_s[c, h] = acc[p, :, 2 * HD + at : 2 * HD + at + HEAD].astype(BF16).T

    def attend(c):
        e = HEAD**-0.5 * LOG2E
        ones = jnp.ones((8, C), BF16)

        def scores(kb):
            return [_dot(k_s[kb, h], q_s[c, :, h * HEAD : (h + 1) * HEAD], 1, 1) for h in range(H)]

        def values(kb, h):
            return jnp.concatenate([vt_s[kb, h], ones], axis=0)

        ok = lax.broadcasted_iota(jnp.int32, (C, C), 1) >= lax.broadcasted_iota(jnp.int32, (C, C), 0)
        for h, s in enumerate(scores(c)):
            s = jnp.where(ok, s, HIDDEN)
            top = s.max(axis=0, keepdims=True)
            top_s[h : h + 1, :] = top
            mix_s[h] = _dot(values(c, h), jnp.exp2((s - top) * e).astype(BF16))

        def block(kb, _):
            weights, keeps = [], []
            for h, s in enumerate(scores(kb)):
                old = top_s[h : h + 1, :]
                top = jnp.maximum(old, s.max(axis=0, keepdims=True))
                top_s[h : h + 1, :] = top
                weights.append(jnp.exp2((s - top) * e).astype(BF16))
                keeps.append(jnp.exp2((old - top) * e))
            for h in range(H):
                mix_s[h] = mix_s[h] * keeps[h] + _dot(values(kb, h), weights[h])

        lax.fori_loop(0, c, block, None)
        for h in range(H):
            out = mix_s[h, :HEAD, :] * (1 / mix_s[h, HEAD : HEAD + 1, :])
            q_s[c, :, h * HEAD : (h + 1) * HEAD] = out.T.astype(BF16)

    def my_rows(w, j):
        return term.at[w, j % 2, pl.ds(pl.multiple_of(r * RB, RB), RB), :]

    def to_partner(w, c, j):
        return remote(pst.at[w, j % 2], xg.at[c, j, pl.ds(RB, RB), :], tp_m.at[w, j % 2], tp_r.at[c, j], partner)

    def run_dn(w, c, j):
        return remote(nst.at[w, j], xg.at[c, j, pl.ds(0, RB), :], ns_m.at[w, j], nr_r.at[c, j], dn)

    def run_up(w, c, j):
        return remote(nst.at[w, j], xg.at[c, j, pl.ds(0, RB), :], ns_m.at[w, j], nr_r.at[c, j], up)

    def run_home(w, j):
        return remote(nst.at[w, j], second.at[j], ns_m.at[w, j], sec_r.at[j], up)

    def y_copy(j):
        return pltpu.make_async_copy(an.at[j], y_ref.at[:, pl.ds(pl.multiple_of(j * KB, KB), KB)], y_m.at[j])

    def wo_start():
        wo_copy(0).start()
        wo_copy(1).start()

    def wo_next(j):
        @pl.when(j + 2 < NB)
        def _():
            wo_copy(j + 2).start()

        wo_copy(j).wait()

    def stage_a(w, c, j):
        @pl.when(j == 0)
        def _():
            pl.semaphore_wait(pcred.at[c], 1)

        tk = min(512, KB)

        def tile(n):
            cols = pl.ds(pl.multiple_of(n * tk, tk), tk)
            term[w, j % 2, :, cols] = _dot(q_s[c], wob[j % 3, :, cols])

        loop(KB // tk, tile)
        theirs = pl.ds(pl.multiple_of((1 - r) * RB, RB), RB)
        pst[w, j % 2] = term[w, j % 2, theirs, :].astype(BF16)
        to_partner(w, c, j).start()

    def stage_b(w, c, j, prior):
        to_partner(w, c, j).wait()
        t = my_rows(w, j)
        t[...] += xg[c, j, RB:, :].astype(F32)

        @pl.when(((c <= z) & (z < 3)) | ((c > z) & (z > 0)))
        def _():
            run_dn(w, c, j).wait_recv()
            t[...] += xg[c, j, :RB, :].astype(F32)

        if prior is None:
            @pl.when(z > 0)
            def _():
                run_home(w, j).wait_recv()
                t[...] += second[j].astype(F32)

            an[j] = (xv[j].astype(F32) + t[...]).astype(BF16)
            y_copy(j).start()
            return

        if prior is not False:
            @pl.when(prior)
            def _():
                run_dn(w, c, j).wait_send()

        @pl.when(j == 0)
        def _():
            pl.semaphore_wait(ncred.at[c], 1)

        nst[w, j] = t[...].astype(BF16)

        @pl.when(c < z)
        def _():
            run_dn(w, c, j).start()

        @pl.when(c == z + 1)
        def _():
            run_home(w, j).start()

        @pl.when(c > z + 1)
        def _():
            run_up(w, c, j).start()

    def stages(j, w, c, prior):
        @pl.when((j >= 0) & (j < NB))
        def _():
            stage_a(w, c, j)

        @pl.when((j > 0) & (j <= NB))
        def _():
            stage_b(w, c, j - 1, prior)

    loop(NB, lambda k: x_copy(k).start())
    rope_copy = pltpu.make_async_copy(rope_ref, rope, rope_m)
    rope_copy.start()
    for g in range(3):
        for copy in w_copies(g):
            copy.start()
    barrier = pltpu.get_barrier_semaphore()
    pl.semaphore_signal(barrier, 1, device_id=partner, device_id_type=MESH)

    @pl.when(z > 0)
    def _():
        pl.semaphore_signal(barrier, 1, device_id=dn, device_id_type=MESH)

    @pl.when(z < 3)
    def _():
        pl.semaphore_signal(barrier, 1, device_id=up, device_id_type=MESH)

    def squares(k, total):
        x_copy(k).wait()
        t = xv[k].astype(F32)
        t = t * t
        for i in range(0, KB, 128):
            total = total + t[:, i : i + 128]
        return total

    total = lax.fori_loop(0, NB, squares, jnp.zeros((RB, 128), F32))
    scale = lax.rsqrt(jnp.sum(total, axis=1, keepdims=True) * (1 / D) + 1e-6)

    def norm(k):
        gain = gain_ref[:, pl.ds(pl.multiple_of(k * KB, KB), KB)].astype(F32)
        t = (xv[k].astype(F32) * scale * gain).astype(BF16)
        an[k] = t
        xg[z, k, pl.ds(pl.multiple_of(r * RB, RB), RB), :] = t

    loop(NB, norm)

    @pl.when((z > 0) & (z < 3))
    def _():
        pl.semaphore_wait(barrier, 3)

    @pl.when((z == 0) | (z == 3))
    def _():
        pl.semaphore_wait(barrier, 2)

    def first_sends(k):
        @pl.when((z == 0) | ((z < 3) & (k < 2 * z - 1)))
        def _():
            gather_up(z, k, an.at[k]).start()

        @pl.when(z > 0)
        def _():
            gather_dn(z, k, an.at[k]).start()

        gather_pa(z, k, an.at[k]).start()

    loop(NB, first_sends)
    acc[...] = jnp.zeros_like(acc)

    def multiply(g, k, chunks):
        for c in chunks:
            got_pa(c, k)

        @pl.when(g + 3 < 3 * NB)
        def _():
            for copy in w_copies(g + 3):
                copy.start()

        for copy in w_copies(g):
            copy.wait()
        project(g, k, chunks)

    c0 = (3 - z) // 3

    def slot0(k):
        @pl.when(k < NB)
        def _():
            comm(0, k)

        @pl.when(k > 0)
        def _():
            multiply(k - 1, k - 1, (z, c0))

    loop(NB + 1, slot0)

    def later_sends(s):
        @pl.when(z == s)
        def _():
            lax.fori_loop(2 * s - 1, NB, lambda k, _: gather_up(z, k, an.at[k]).start(), None)

    later_sends(1)
    rope_copy.wait()
    turn(0, z)
    turn(1, c0)
    freed(c0)

    pl.semaphore_signal(pcred.at[z], 1, device_id=partner, device_id_type=MESH)

    @pl.when(z < 3)
    def _():
        pl.semaphore_signal(ncred.at[z], 1, device_id=up, device_id_type=MESH)

    @pl.when(z > 0)
    def _():
        pl.semaphore_signal(ncred.at[z], 1, device_id=dn, device_id_type=MESH)

    firsts = (0, 2 - z // 2, 3 - z // 3, 4)
    lax.fori_loop(firsts[0], firsts[1], lambda c, _: attend(c), None)

    two = (z % 3) // 2
    one = (z % 3) % 2
    for s in (1, 2):
        cp = (2 - z // 2, 3 - z // 3)[s - 1]
        cs = (1 - (z + 1) // 3, 2 - z // 2)[s - 1]
        lag = (LAGS[0] * two, LAGS[1] * one + LAGS[2] * two)[s - 1]
        summing = (z != 1) if s == 1 else (z >= 0)
        acc[0] = jnp.zeros_like(acc[0])

        @pl.when(summing)
        def _():
            wo_start()

        def sums(j):
            @pl.when(summing)
            def _():
                @pl.when((j >= 0) & (j < NB))
                def _():
                    wo_next(j)

                if s == 1:
                    stages(j, 0, cs, False)
                else:
                    stages(j, 0, cs, z != 1)

                    @pl.when(z == 1)
                    def _():
                        stages(j, 1, 0, False)

        def slot(k):
            g = s * NB + k

            @pl.when(k < NB)
            def _():
                comm(s, k)

            @pl.when(k > 0)
            def _():
                multiply(g - 1, k - 1, (cp,))

            sums(k - lag)

        loop(NB + 1, slot)
        if s == 1:
            later_sends(2)
        turn(0, cp)
        if s == 2:
            freed(cp)
        lax.fori_loop(firsts[s], firsts[s + 1], lambda c, _: attend(c), None)
        if s == 1:
            freed(cp)
        loop(lag, lambda k: sums(NB + 1 + k - lag))

    @pl.when((z == 0) | (z == 3))
    def _():
        wo_start()

        def last(j):
            @pl.when(j < NB)
            def _():
                wo_next(j)

            stages(j, 0, 3 - z // 3, z >= 0)

        loop(NB + 1, last)

    wo_start()

    def own_sent(k):
        gather_pa(z, k, an.at[k]).wait_send()

        @pl.when(z > 0)
        def _():
            gather_dn(z, k, an.at[k]).wait_send()

        @pl.when(z < 3)
        def _():
            gather_up(z, k, an.at[k]).wait_send()

    loop(NB, own_sent)

    def home(j):
        @pl.when(j < NB)
        def _():
            wo_next(j)

        @pl.when((z == 1) | (z == 2))
        def _():
            stages(j, 0, 3, z >= 0)

        stages(j, 1, z, None)

    loop(NB + 1, home)

    def rest(k):
        y_copy(k).wait()
        run_dn(0, 0, k).wait_send()

        @pl.when(z == 1)
        def _():
            run_dn(1, 0, k).wait_send()

    loop(NB, rest)


def _fused(x, gain, wq, wk, wv, wo, rope):
    RB, D = x.shape
    HD = wq.shape[1]
    H, KB, C = HD // HEAD, D // NB, 2 * RB
    dma = pltpu.SemaphoreType.DMA
    return pl.pallas_call(
        _kernel,
        out_shape=jax.ShapeDtypeStruct((RB, D), BF16),
        in_specs=[pl.BlockSpec(memory_space=m) for m in (pl.ANY, pltpu.VMEM, pl.ANY, pl.ANY, pl.ANY, pl.ANY, pl.ANY)],
        out_specs=pl.BlockSpec(memory_space=pl.ANY),
        scratch_shapes=[
            pltpu.VMEM((NB, RB, KB), BF16),
            pltpu.VMEM((NB, RB, KB), BF16),
            pltpu.VMEM(rope.shape, F32),
            pltpu.VMEM((4, NB, C, KB), BF16),
            pltpu.VMEM((4, 3, KB, HD), BF16),
            pltpu.VMEM((3, HD, KB), BF16),
            pltpu.VMEM((2, C, 3 * HD), F32),
            pltpu.VMEM((4, C, HD), BF16),
            pltpu.VMEM((4, H, C, HEAD), BF16),
            pltpu.VMEM((4, H, HEAD, C), BF16),
            pltpu.VMEM((H, HEAD + 8, C), F32),
            pltpu.VMEM((H, C), F32),
            pltpu.VMEM((NB, RB, KB), BF16),
            pltpu.VMEM((2, 2, C, KB), F32),
            pltpu.VMEM((2, 2, RB, KB), BF16),
            pltpu.VMEM((2, NB, RB, KB), BF16),
            dma((NB,)),
            dma,
            dma((4, 3)),
            dma((3,)),
            dma((4, NB)),
            dma((4, NB)),
            dma((4, NB)),
            dma((4, NB)),
            dma((4, NB)),
            dma((2, 2)),
            dma((4, NB)),
            dma((2, NB)),
            dma((4, NB)),
            dma((NB,)),
            dma((NB,)),
            pltpu.SemaphoreType.REGULAR((4,)),
            pltpu.SemaphoreType.REGULAR((4,)),
        ],
        compiler_params=pltpu.CompilerParams(collective_id=0, has_side_effects=True, vmem_limit_bytes=67043328),
    )(x, gain.reshape(1, D), wq, wk, wv, wo, rope)


def _rope(rows):
    half = HEAD // 2
    angle = np.arange(rows, dtype=np.float32)[:, None] * np.float32(THETA) ** (-np.arange(half, dtype=np.float32) / np.float32(half))
    return np.concatenate([np.cos(angle), np.sin(angle)], 1).astype(np.float32)


def solution(mesh):
    def step(x, gain, wq, wk, wv, wo):
        return _fused(x, gain, wq, wk, wv, wo, jnp.asarray(_rope(x.shape[0] * mesh.shape["tp"])))

    tokens, columns = P(("dp", "tp"), None), P(None, "tp")
    return jax.shard_map(
        step,
        mesh=mesh,
        in_specs=(tokens, P(None), columns, columns, columns, P("tp", None)),
        out_specs=tokens,
        check_vma=False,
    )
```

```python
import jax
import jax.numpy as jnp
import numpy as np
from jax import lax
from jax.experimental import pallas as pl
from jax.experimental.pallas import tpu as pltpu
from jax.sharding import PartitionSpec as P

HEAD = 128
THETA = 10000
NB = 16
HIDDEN = -2e30
LOG2E = 1.4426950408889634
LAGS = (6, 5, 10)
MESH = pl.DeviceIdType.MESH
F32, BF16 = jnp.float32, jnp.bfloat16


def _dot(a, b, ca=1, cb=0):
    return lax.dot_general(a, b, (((ca,), (cb,)), ((), ())), preferred_element_type=F32)


def _kernel(x_ref, gain_ref, wq_ref, wk_ref, wv_ref, wo_ref, rope_ref, y_ref,
            xv, an, rope, xg, wbuf, wob, acc, q_s, k_s, vt_s, mix_s, top_s, second, term, pst, nst,
            x_m, rope_m, w_m, wo_m, up_m, dn_m, pa_m, nb_r, pa_r, tp_m, ns_m, sec_r, y_m, pcred, ncred):
    RB, D = x_ref.shape
    HD = wq_ref.shape[1]
    H = HD // HEAD
    KB = D // NB
    C = 2 * RB
    TN = HD
    me = lax.axis_index("tp")
    z, r = me // 2, me % 2
    up, dn, partner = {"tp": me + 2}, {"tp": me - 2}, {"tp": me + 1 - 2 * r}
    weights = (wq_ref, wk_ref, wv_ref)

    def remote(src, dst, send, recv, to):
        return pltpu.make_async_remote_copy(src_ref=src, dst_ref=dst, send_sem=send, recv_sem=recv, device_id=to, device_id_type=MESH)

    def half(c, k, h):
        return xg.at[c, k, pl.ds(pl.multiple_of(h * RB, RB), RB), :]

    def gather_up(c, k, src):
        return remote(src, half(c, k, r), up_m.at[c], nb_r.at[c, k], up)

    def gather_dn(c, k, src):
        return remote(src, half(c, k, r), dn_m.at[c], nb_r.at[c, k], dn)

    def gather_pa(c, k, src):
        return remote(src, half(c, k, r), pa_m.at[c], pa_r.at[c, k], partner)

    def all_sent(c, sem):
        remote(an, xg.at[c, :, pl.ds(0, RB), :], sem.at[c], nb_r.at[c, 0], partner).wait_send()

    def got_pa(c, k):
        remote(half(c, k, 1 - r), half(c, k, 1 - r), pa_m.at[c], pa_r.at[c, k], partner).wait_recv()

    def block(k):
        return pl.ds(pl.multiple_of(k * KB, KB), KB)

    def w_copies(g):
        at = pl.ds(pl.multiple_of((g % NB) * KB, KB), KB)
        return [pltpu.make_async_copy(weights[i].at[at, :], wbuf.at[g % 4, i], w_m.at[g % 4, i]) for i in range(3)]

    def wo_copy(j):
        return pltpu.make_async_copy(wo_ref.at[:, block(j)], wob.at[j % 3], wo_m.at[j % 3])

    def loop(n, body):
        lax.fori_loop(0, n, lambda i, _: body(i), None)

    def comm(s, k):
        @pl.when(z > s)
        def _():
            gather_up(s, k, half(s, k, r)).wait_recv()

            @pl.when(z < 3)
            def _():
                gather_up(s, k, half(s, k, r)).start()

            gather_pa(s, k, half(s, k, r)).start()

        d = z + 1 + s

        @pl.when(d <= 3)
        def _():
            gather_dn(d, k, half(d, k, r)).wait_recv()

            @pl.when(z > 0)
            def _():
                gather_dn(d, k, half(d, k, r)).start()

            gather_pa(d, k, half(d, k, r)).start()

    def freed(c):
        @pl.when((z > c) & (z < 3))
        def _():
            all_sent(c, up_m)

        @pl.when((z < c) & (z > 0))
        def _():
            all_sent(c, dn_m)

        all_sent(c, pa_m)
        pl.semaphore_signal(pcred.at[c], 1, device_id=partner, device_id_type=MESH)

        @pl.when((c <= z) & (z < 3))
        def _():
            pl.semaphore_signal(ncred.at[c], 1, device_id=up, device_id_type=MESH)

        @pl.when((c >= z) & (z > 0))
        def _():
            pl.semaphore_signal(ncred.at[c], 1, device_id=dn, device_id_type=MESH)

    def project(g, k, chunks, first, last):
        n = HD // TN

        def tile(t, _):
            i, at = t // n, pl.multiple_of((t % n) * TN, TN)
            w = wbuf[g % 4, i, :, pl.ds(at, TN)]
            cols = pl.ds(pl.multiple_of(t * TN, TN), TN)
            for p, c in enumerate(chunks):
                acc[p, :, cols] += _dot(xg[c, k], w)

        lax.fori_loop(first * n, last * n, tile, None)

    def turn(p, c):
        rows = pl.ds(pl.multiple_of(c * C, C), C)
        cs = rope[rows, :]
        sc = pltpu.roll(cs, HEAD // 2, 1)
        first = lax.broadcasted_iota(jnp.int32, cs.shape, 1) < HEAD // 2
        cos, sin = jnp.where(first, cs, sc), jnp.where(first, -sc, cs)

        def turned(t):
            t = t.astype(BF16).astype(F32)
            return (t * cos + pltpu.roll(t, HEAD // 2, 1) * sin).astype(BF16)

        for h in range(H):
            at = h * HEAD
            q_s[c, :, at : at + HEAD] = turned(acc[p, :, at : at + HEAD])
            k_s[c, h] = turned(acc[p, :, HD + at : HD + at + HEAD])
            vt_s[c, h] = acc[p, :, 2 * HD + at : 2 * HD + at + HEAD].astype(BF16).T

    def attend(c):
        e = HEAD**-0.5 * LOG2E
        ones = jnp.ones((8, C), BF16)

        def scores(kb):
            return [_dot(k_s[kb, h], q_s[c, :, h * HEAD : (h + 1) * HEAD], 1, 1) for h in range(H)]

        def values(kb, h):
            return jnp.concatenate([vt_s[kb, h], ones], axis=0)

        ok = lax.broadcasted_iota(jnp.int32, (C, C), 1) >= lax.broadcasted_iota(jnp.int32, (C, C), 0)
        for h, s in enumerate(scores(c)):
            s = jnp.where(ok, s, HIDDEN)
            top = s.max(axis=0, keepdims=True)
            top_s[h : h + 1, :] = top
            mix_s[h] = _dot(values(c, h), jnp.exp2((s - top) * e).astype(BF16))

        def block(kb, _):
            weights, keeps = [], []
            for h, s in enumerate(scores(kb)):
                old = top_s[h : h + 1, :]
                top = jnp.maximum(old, s.max(axis=0, keepdims=True))
                top_s[h : h + 1, :] = top
                weights.append(jnp.exp2((s - top) * e).astype(BF16))
                keeps.append(jnp.exp2((old - top) * e))
            for h in range(H):
                mix_s[h] = mix_s[h] * keeps[h] + _dot(values(kb, h), weights[h])

        lax.fori_loop(0, c, block, None)
        for h in range(H):
            out = mix_s[h, :HEAD, :] * (1 / mix_s[h, HEAD : HEAD + 1, :])
            q_s[c, :, h * HEAD : (h + 1) * HEAD] = out.T.astype(BF16)

    def slot_of(w, j):
        return 2 + j % 4 if w else j % 2

    def my_rows(w, j):
        return term.at[slot_of(w, j), pl.ds(pl.multiple_of(r * RB, RB), RB), :]

    def to_partner(w, c, j):
        return remote(pst.at[slot_of(w, j)], xg.at[c, j, pl.ds(RB, RB), :], tp_m.at[slot_of(w, j)], pa_r.at[c, j], partner)

    def run_dn(w, c, j):
        return remote(nst.at[w, j], xg.at[c, j, pl.ds(0, RB), :], ns_m.at[w * NB + j * (1 - w)], nb_r.at[c, j], dn)

    def run_up(w, c, j):
        return remote(nst.at[w, j], xg.at[c, j, pl.ds(0, RB), :], ns_m.at[w * NB + j * (1 - w)], nb_r.at[c, j], up)

    def run_home(w, j):
        return remote(nst.at[w, j], second.at[j], ns_m.at[w * NB + j * (1 - w)], sec_r.at[j], up)

    def y_copy(j):
        return pltpu.make_async_copy(an.at[j], y_ref.at[:, block(j)], y_m)

    def wo_start(when):
        @pl.when(when)
        def _():
            wo_copy(0).start()
            wo_copy(1).start()

    def wo_next(j):
        @pl.when(j + 2 < NB)
        def _():
            wo_copy(j + 2).start()

        wo_copy(j).wait()

    def stage_a(w, c, j):
        @pl.when(j == 0)
        def _():
            pl.semaphore_wait(pcred.at[c], 1)

        tk = min(512, KB)

        def tile(n):
            cols = pl.ds(pl.multiple_of(n * tk, tk), tk)
            term[slot_of(w, j), :, cols] = _dot(q_s[c], wob[j % 3, :, cols])

        loop(KB // tk, tile)
        theirs = pl.ds(pl.multiple_of((1 - r) * RB, RB), RB)
        pst[slot_of(w, j)] = term[slot_of(w, j), theirs, :].astype(BF16)
        to_partner(w, c, j).start()

    def stage_b(w, c, j, prior):
        to_partner(w, c, j).wait()
        t = my_rows(w, j)
        t[...] += xg[c, j, RB:, :].astype(F32)

        @pl.when(((c <= z) & (z < 3)) | ((c > z) & (z > 0)))
        def _():
            run_dn(w, c, j).wait_recv()
            t[...] += xg[c, j, :RB, :].astype(F32)

        if prior is None:
            @pl.when(z > 0)
            def _():
                run_home(w, j).wait_recv()
                t[...] += second[j].astype(F32)

            an[j] = (xv[:, block(j)].astype(F32) + t[...]).astype(BF16)
            y_copy(j).start()
            return

        if prior is not False:
            @pl.when(prior)
            def _():
                run_dn(w, c, j).wait_send()

        @pl.when(j == 0)
        def _():
            pl.semaphore_wait(ncred.at[c], 1)

        nst[w, j] = t[...].astype(BF16)

        @pl.when(c < z)
        def _():
            run_dn(w, c, j).start()

        @pl.when(c == z + 1)
        def _():
            run_home(w, j).start()

        @pl.when(c > z + 1)
        def _():
            run_up(w, c, j).start()

    def stages(j, w, c, prior, late=1):
        @pl.when((j >= 0) & (j < NB))
        def _():
            stage_a(w, c, j)

        @pl.when((j >= late) & (j < NB + late))
        def _():
            stage_b(w, c, j - late, prior)

    loop(NB, lambda k: pltpu.make_async_copy(x_ref.at[:, block(k)], xv.at[:, block(k)], x_m).start())
    barrier = pltpu.get_barrier_semaphore()
    pl.semaphore_signal(barrier, 1, device_id=partner, device_id_type=MESH)

    @pl.when(z > 0)
    def _():
        pl.semaphore_signal(barrier, 1, device_id=dn, device_id_type=MESH)

    @pl.when(z < 3)
    def _():
        pl.semaphore_signal(barrier, 1, device_id=up, device_id_type=MESH)

    def squares(k, total):
        t = xv[:, block(k)].astype(F32)
        t = t * t
        for i in range(0, KB, 128):
            total = total + t[:, i : i + 128]
        return total

    pltpu.make_async_copy(x_ref, xv, x_m).wait()
    rope_copy = pltpu.make_async_copy(rope_ref, rope, rope_m)
    rope_copy.start()
    for g in range(3):
        for copy in w_copies(g):
            copy.start()
    total = lax.fori_loop(0, NB, squares, jnp.zeros((RB, 128), F32))
    scale = lax.rsqrt(jnp.sum(total, axis=1, keepdims=True) * (1 / D) + 1e-6)

    def norm(k):
        gain = gain_ref[block(k)].astype(F32).reshape(1, KB)
        t = (xv[:, block(k)].astype(F32) * scale * gain).astype(BF16)
        an[k] = t
        xg[z, k, pl.ds(pl.multiple_of(r * RB, RB), RB), :] = t

    loop(NB, norm)

    @pl.when((z > 0) & (z < 3))
    def _():
        pl.semaphore_wait(barrier, 3)

    @pl.when((z == 0) | (z == 3))
    def _():
        pl.semaphore_wait(barrier, 2)

    def first_sends(k):
        @pl.when((z == 0) | ((z < 3) & (k < 2 * z - 1)))
        def _():
            gather_up(z, k, an.at[k]).start()

        @pl.when(z > 0)
        def _():
            gather_dn(z, k, an.at[k]).start()

    loop(NB, first_sends)
    loop(2, lambda k: gather_pa(z, k, an.at[k]).start())
    acc[...] = jnp.zeros_like(acc)

    def multiply(g, k, chunks):
        for c in chunks:
            got_pa(c, k)

        @pl.when(g + 3 < 3 * NB)
        def _():
            for copy in w_copies(g + 3):
                copy.start()

        for copy in w_copies(g):
            copy.wait()
        project(g, k, chunks, 0, 1)

    c0 = (3 - z) // 3

    def slot0(k):
        @pl.when(k < NB)
        def _():
            comm(0, k)

        @pl.when(k + 2 < NB)
        def _():
            gather_pa(z, k + 2, an.at[k + 2]).start()

        @pl.when(k > 0)
        def _():
            project(k - 1, k - 1, (z, c0), 1, 3)

        @pl.when(k < NB)
        def _():
            multiply(k, k, (z, c0))

    loop(NB + 1, slot0)

    def later_sends(s):
        @pl.when(z == s)
        def _():
            lax.fori_loop(2 * s - 1, NB, lambda k, _: gather_up(z, k, an.at[k]).start(), None)

    later_sends(1)
    wo_start(z != 1)
    rope_copy.wait()
    turn(0, z)
    turn(1, c0)
    freed(c0)

    pl.semaphore_signal(pcred.at[z], 1, device_id=partner, device_id_type=MESH)

    @pl.when(z < 3)
    def _():
        pl.semaphore_signal(ncred.at[z], 1, device_id=up, device_id_type=MESH)

    @pl.when(z > 0)
    def _():
        pl.semaphore_signal(ncred.at[z], 1, device_id=dn, device_id_type=MESH)

    outer = (z == 0) | (z == 3)
    firsts = (0, 2 - z // 2, 3 - z // 3, 4)
    attend(1 - z // 2)

    two = (z % 3) // 2
    one = (z % 3) % 2
    for s in (1, 2):
        cp = (2 - z // 2, 3 - z // 3)[s - 1]
        cs = (1 - (z + 1) // 3, 2 - z // 2)[s - 1]
        lag = (LAGS[0] * two, LAGS[1] * one + LAGS[2] * two)[s - 1]
        summing = (z != 1) if s == 1 else (z >= 0)
        acc[0] = jnp.zeros_like(acc[0])

        def sums(j):
            @pl.when(summing)
            def _():
                @pl.when((j >= 0) & (j < NB))
                def _():
                    wo_next(j)

                if s == 1:
                    stages(j, 0, cs, False)
                else:
                    stages(j, 0, cs, z != 1)

                    @pl.when(z == 1)
                    def _():
                        stages(j, 1, 0, False)

        def slot(k):
            g = s * NB + k

            @pl.when(k < NB)
            def _():
                comm(s, k)

            sums(k - lag)

            @pl.when(k > 0)
            def _():
                project(g - 1, k - 1, (cp,), 1, 3)

            @pl.when(k < NB)
            def _():
                multiply(g, k, (cp,))

        loop(NB + 1, slot)
        wo_start(outer)
        if s == 1:
            later_sends(2)
        turn(0, cp)
        if s == 2:
            freed(cp)
        lax.fori_loop(firsts[s], firsts[s + 1], lambda c, _: attend(c), None)
        if s == 1:
            freed(cp)

            @pl.when(z == 1)
            def _():
                attend(0)

        loop(lag, lambda k: sums(NB + 1 + k - lag))
        wo_start(~outer)

    @pl.when(outer)
    def _():
        def last(j):
            @pl.when(j < NB)
            def _():
                wo_next(j)

            stages(j, 0, 3 - z // 3, z >= 0)

        loop(NB + 1, last)
        wo_start(outer)

        @pl.when(z == 0)
        def _():
            attend(0)


    all_sent(z, pa_m)

    @pl.when(z > 0)
    def _():
        all_sent(z, dn_m)

    @pl.when(z < 3)
    def _():
        all_sent(z, up_m)

    def home(j):
        @pl.when(j < NB)
        def _():
            wo_next(j)

        @pl.when((z == 1) | (z == 2))
        def _():
            stages(j, 0, 3, z >= 0)

        stages(j, 1, z, None, 3)

    loop(NB + 3, home)

    loop(NB, lambda k: run_dn(0, 0, k).wait_send())

    @pl.when(z == 1)
    def _():
        remote(nst.at[1], xg.at[0, :, pl.ds(0, RB), :], ns_m.at[NB], nb_r.at[0, 0], dn).wait_send()

    pltpu.make_async_copy(y_ref, y_ref, y_m).wait()


def _fused(x, gain, wq, wk, wv, wo, rope):
    RB, D = x.shape
    HD = wq.shape[1]
    H, KB, C = HD // HEAD, D // NB, 2 * RB
    dma = pltpu.SemaphoreType.DMA
    return pl.pallas_call(
        _kernel,
        out_shape=jax.ShapeDtypeStruct((RB, D), BF16),
        in_specs=[pl.BlockSpec(memory_space=m) for m in (pl.ANY, pltpu.VMEM, pl.ANY, pl.ANY, pl.ANY, pl.ANY, pl.ANY)],
        out_specs=pl.BlockSpec(memory_space=pl.ANY),
        scratch_shapes=[
            pltpu.VMEM((RB, D), BF16),
            pltpu.VMEM((NB, RB, KB), BF16),
            pltpu.VMEM(rope.shape, F32),
            pltpu.VMEM((4, NB, C, KB), BF16),
            pltpu.VMEM((4, 3, KB, HD), BF16),
            pltpu.VMEM((3, HD, KB), BF16),
            pltpu.VMEM((2, C, 3 * HD), F32),
            pltpu.VMEM((4, C, HD), BF16),
            pltpu.VMEM((4, H, C, HEAD), BF16),
            pltpu.VMEM((4, H, HEAD, C), BF16),
            pltpu.VMEM((H, HEAD + 8, C), F32),
            pltpu.VMEM((H, C), F32),
            pltpu.VMEM((NB, RB, KB), BF16),
            pltpu.VMEM((6, C, KB), F32),
            pltpu.VMEM((6, RB, KB), BF16),
            pltpu.VMEM((2, NB, RB, KB), BF16),
            dma,
            dma,
            dma((4, 3)),
            dma((3,)),
            dma((4,)),
            dma((4,)),
            dma((4,)),
            dma((4, NB)),
            dma((4, NB)),
            dma((6,)),
            dma((NB + 1,)),
            dma((NB,)),
            dma,
            pltpu.SemaphoreType.REGULAR((4,)),
            pltpu.SemaphoreType.REGULAR((4,)),
        ],
        compiler_params=pltpu.CompilerParams(collective_id=0, has_side_effects=True, vmem_limit_bytes=67043328),
    )(x, gain, wq, wk, wv, wo, rope)


def _rope(rows):
    half = HEAD // 2
    angle = np.arange(rows, dtype=np.float32)[:, None] * np.float32(THETA) ** (-np.arange(half, dtype=np.float32) / np.float32(half))
    return np.concatenate([np.cos(angle), np.sin(angle)], 1).astype(np.float32)


def solution(mesh):
    def step(x, gain, wq, wk, wv, wo):
        return _fused(x, gain, wq, wk, wv, wo, jnp.asarray(_rope(x.shape[0] * mesh.shape["tp"])))

    tokens, columns = P(("dp", "tp"), None), P(None, "tp")
    return jax.shard_map(
        step,
        mesh=mesh,
        in_specs=(tokens, P(None), columns, columns, columns, P("tp", None)),
        out_specs=tokens,
        check_vma=False,
    )
```

```python
import jax
import jax.numpy as jnp
import numpy as np
from jax import lax
from jax.experimental import pallas as pl
from jax.experimental.pallas import tpu as pltpu
from jax.sharding import PartitionSpec as P

HEAD = 128
THETA = 10000
NB = 16
HIDDEN = -2e30
LOG2E = 1.4426950408889634
LAGS = (6, 5, 10)
MESH = pl.DeviceIdType.MESH
F32, BF16 = jnp.float32, jnp.bfloat16


def _dot(a, b, ca=1, cb=0):
    return lax.dot_general(a, b, (((ca,), (cb,)), ((), ())), preferred_element_type=F32)


def _kernel(x_ref, gain_ref, wq_ref, wk_ref, wv_ref, wo_ref, rope_ref, y_ref,
            xv, an, gain_v, rope, xg, wbuf, wob, acc, q_s, k_s, vt_s, mix_s, top_s, second, term, pst, nst,
            x_m, gain_m, rope_m, w_m, wo_m, up_m, dn_m, pa_m, nb_r, pa_r, tp_m, ns_m, sec_r, pcred, ncred):
    RB, D = x_ref.shape
    HD = wq_ref.shape[1]
    H = HD // HEAD
    KB = D // NB
    C = 2 * RB
    TN = HD
    me = lax.axis_index("tp")
    z, r = me // 2, me % 2
    up, dn, partner = {"tp": me + 2}, {"tp": me - 2}, {"tp": me + 1 - 2 * r}
    weights = (wq_ref, wk_ref, wv_ref)

    def remote(src, dst, send, recv, to):
        return pltpu.make_async_remote_copy(src_ref=src, dst_ref=dst, send_sem=send, recv_sem=recv, device_id=to, device_id_type=MESH)

    def half(c, k, h):
        return xg.at[c, k, pl.ds(pl.multiple_of(h * RB, RB), RB), :]

    def gather_up(c, k, src):
        return remote(src, half(c, k, r), up_m.at[c], nb_r.at[c, k], up)

    def gather_dn(c, k, src):
        return remote(src, half(c, k, r), dn_m.at[c], nb_r.at[c, k], dn)

    def gather_pa(c, k, src):
        return remote(src, half(c, k, r), pa_m.at[c], pa_r.at[c, k], partner)

    def all_sent(c, sem):
        remote(an, xg.at[c, :, pl.ds(0, RB), :], sem.at[c], nb_r.at[c, 0], partner).wait_send()

    def got_pa(c, k):
        remote(half(c, k, 1 - r), half(c, k, 1 - r), pa_m.at[c], pa_r.at[c, k], partner).wait_recv()

    def block(k):
        return pl.ds(pl.multiple_of(k * KB, KB), KB)

    def w_copies(g):
        at = pl.ds(pl.multiple_of((g % NB) * KB, KB), KB)
        return [pltpu.make_async_copy(weights[i].at[at, :], wbuf.at[g % 4, i], w_m.at[g % 4, i]) for i in range(3)]

    def wo_copy(j):
        return pltpu.make_async_copy(wo_ref.at[:, block(j)], wob.at[j % 3], wo_m.at[j % 3])

    def loop(n, body):
        lax.fori_loop(0, n, lambda i, _: body(i), None)

    def comm(s, k):
        @pl.when(z > s)
        def _():
            gather_up(s, k, half(s, k, r)).wait_recv()

            @pl.when(z < 3)
            def _():
                gather_up(s, k, half(s, k, r)).start()

            gather_pa(s, k, half(s, k, r)).start()

        d = z + 1 + s

        @pl.when(d <= 3)
        def _():
            gather_dn(d, k, half(d, k, r)).wait_recv()

            @pl.when(z > 0)
            def _():
                gather_dn(d, k, half(d, k, r)).start()

            gather_pa(d, k, half(d, k, r)).start()

    def freed(c):
        @pl.when((z > c) & (z < 3))
        def _():
            all_sent(c, up_m)

        @pl.when((z < c) & (z > 0))
        def _():
            all_sent(c, dn_m)

        all_sent(c, pa_m)
        pl.semaphore_signal(pcred.at[c], 1, device_id=partner, device_id_type=MESH)

        @pl.when((c <= z) & (z < 3))
        def _():
            pl.semaphore_signal(ncred.at[c], 1, device_id=up, device_id_type=MESH)

        @pl.when((c >= z) & (z > 0))
        def _():
            pl.semaphore_signal(ncred.at[c], 1, device_id=dn, device_id_type=MESH)

    def project(g, k, chunks, first, last):
        n = HD // TN

        def tile(t, _):
            i, at = t // n, pl.multiple_of((t % n) * TN, TN)
            w = wbuf[g % 4, i, :, pl.ds(at, TN)]
            cols = pl.ds(pl.multiple_of(t * TN, TN), TN)
            for p, c in enumerate(chunks):
                acc[p, :, cols] += _dot(xg[c, k], w)

        lax.fori_loop(first * n, last * n, tile, None)

    def turn(p, c):
        rows = pl.ds(pl.multiple_of(c * C, C), C)
        cs = rope[rows, :]
        sc = pltpu.roll(cs, HEAD // 2, 1)
        first = lax.broadcasted_iota(jnp.int32, cs.shape, 1) < HEAD // 2
        cos, sin = jnp.where(first, cs, sc), jnp.where(first, -sc, cs)

        def turned(t):
            t = t.astype(BF16).astype(F32)
            return (t * cos + pltpu.roll(t, HEAD // 2, 1) * sin).astype(BF16)

        for h in range(H):
            at = h * HEAD
            q_s[c, :, at : at + HEAD] = turned(acc[p, :, at : at + HEAD])
            k_s[c, h] = turned(acc[p, :, HD + at : HD + at + HEAD])
            vt_s[c, h] = acc[p, :, 2 * HD + at : 2 * HD + at + HEAD].astype(BF16).T

    def attend(c):
        e = HEAD**-0.5 * LOG2E
        ones = jnp.ones((8, C), BF16)

        def scores(kb):
            return [_dot(k_s[kb, h], q_s[c, :, h * HEAD : (h + 1) * HEAD], 1, 1) for h in range(H)]

        def values(kb, h):
            return jnp.concatenate([vt_s[kb, h], ones], axis=0)

        ok = lax.broadcasted_iota(jnp.int32, (C, C), 1) >= lax.broadcasted_iota(jnp.int32, (C, C), 0)
        for h, s in enumerate(scores(c)):
            s = jnp.where(ok, s, HIDDEN)
            top = s.max(axis=0, keepdims=True)
            top_s[h : h + 1, :] = top
            mix_s[h] = _dot(values(c, h), jnp.exp2((s - top) * e).astype(BF16))

        def block(kb, _):
            weights, keeps = [], []
            for h, s in enumerate(scores(kb)):
                old = top_s[h : h + 1, :]
                top = jnp.maximum(old, s.max(axis=0, keepdims=True))
                top_s[h : h + 1, :] = top
                weights.append(jnp.exp2((s - top) * e).astype(BF16))
                keeps.append(jnp.exp2((old - top) * e))
            for h in range(H):
                mix_s[h] = mix_s[h] * keeps[h] + _dot(values(kb, h), weights[h])

        lax.fori_loop(0, c, block, None)
        for h in range(H):
            out = mix_s[h, :HEAD, :] * (1 / mix_s[h, HEAD : HEAD + 1, :])
            q_s[c, :, h * HEAD : (h + 1) * HEAD] = out.T.astype(BF16)

    def slot_of(w, j):
        return 2 + j % 4 if w else j % 2

    def my_rows(w, j):
        return term.at[slot_of(w, j), pl.ds(pl.multiple_of(r * RB, RB), RB), :]

    def to_partner(w, c, j):
        return remote(pst.at[slot_of(w, j)], xg.at[c, j, pl.ds(RB, RB), :], tp_m.at[slot_of(w, j)], pa_r.at[c, j], partner)

    def staged(w):
        return an if w else nst

    def run_dn(w, c, j):
        return remote(staged(w).at[j], xg.at[c, j, pl.ds(0, RB), :], ns_m.at[w * NB + j * (1 - w)], nb_r.at[c, j], dn)

    def run_up(w, c, j):
        return remote(staged(w).at[j], xg.at[c, j, pl.ds(0, RB), :], ns_m.at[w * NB + j * (1 - w)], nb_r.at[c, j], up)

    def run_home(w, j):
        return remote(staged(w).at[j], second.at[j], ns_m.at[w * NB + j * (1 - w)], sec_r.at[j], up)

    def wo_start(when):
        @pl.when(when)
        def _():
            wo_copy(0).start()
            wo_copy(1).start()

    def wo_next(j):
        @pl.when(j + 2 < NB)
        def _():
            wo_copy(j + 2).start()

        wo_copy(j).wait()

    def stage_a(w, c, j):
        @pl.when(j == 0)
        def _():
            pl.semaphore_wait(pcred.at[c], 1)

        tk = min(512, KB)

        def tile(n):
            cols = pl.ds(pl.multiple_of(n * tk, tk), tk)
            term[slot_of(w, j), :, cols] = _dot(q_s[c], wob[j % 3, :, cols])

        loop(KB // tk, tile)
        theirs = pl.ds(pl.multiple_of((1 - r) * RB, RB), RB)
        pst[slot_of(w, j)] = term[slot_of(w, j), theirs, :].astype(BF16)
        to_partner(w, c, j).start()

    def stage_b(w, c, j, prior):
        to_partner(w, c, j).wait()
        t = my_rows(w, j)
        t[...] += xg[c, j, RB:, :].astype(F32)

        @pl.when(((c <= z) & (z < 3)) | ((c > z) & (z > 0)))
        def _():
            run_dn(w, c, j).wait_recv()
            t[...] += xg[c, j, :RB, :].astype(F32)

        if prior is None:
            @pl.when(z > 0)
            def _():
                run_home(w, j).wait_recv()
                t[...] += second[j].astype(F32)

            y_ref[:, block(j)] = (xv[:, block(j)].astype(F32) + t[...]).astype(BF16)
            return

        if prior is not False:
            @pl.when(prior)
            def _():
                run_dn(w, c, j).wait_send()

        @pl.when(j == 0)
        def _():
            pl.semaphore_wait(ncred.at[c], 1)

        staged(w)[j] = t[...].astype(BF16)

        @pl.when(c < z)
        def _():
            run_dn(w, c, j).start()

        @pl.when(c == z + 1)
        def _():
            run_home(w, j).start()

        @pl.when(c > z + 1)
        def _():
            run_up(w, c, j).start()

    def stages(j, w, c, prior, late=1):
        @pl.when((j >= 0) & (j < NB))
        def _():
            stage_a(w, c, j)

        @pl.when((j >= late) & (j < NB + late))
        def _():
            stage_b(w, c, j - late, prior)

    loop(NB, lambda k: pltpu.make_async_copy(x_ref.at[:, block(k)], xv.at[:, block(k)], x_m).start())
    gain_copy = pltpu.make_async_copy(gain_ref, gain_v, gain_m)
    gain_copy.start()
    barrier = pltpu.get_barrier_semaphore()
    pl.semaphore_signal(barrier, 1, device_id=partner, device_id_type=MESH)

    @pl.when(z > 0)
    def _():
        pl.semaphore_signal(barrier, 1, device_id=dn, device_id_type=MESH)

    @pl.when(z < 3)
    def _():
        pl.semaphore_signal(barrier, 1, device_id=up, device_id_type=MESH)

    def squares(k, total):
        t = xv[:, block(k)].astype(F32)
        t = t * t
        for i in range(0, KB, 128):
            total = total + t[:, i : i + 128]
        return total

    pltpu.make_async_copy(x_ref, xv, x_m).wait()
    total = lax.fori_loop(0, NB, squares, jnp.zeros((RB, 128), F32))
    scale = lax.rsqrt(jnp.sum(total, axis=1, keepdims=True) * (1 / D) + 1e-6)

    def norm(k):
        gain = gain_v[block(k)].astype(F32).reshape(1, KB)
        t = (xv[:, block(k)].astype(F32) * scale * gain).astype(BF16)
        an[k] = t
        xg[z, k, pl.ds(pl.multiple_of(r * RB, RB), RB), :] = t

    def first_sends(k):
        @pl.when((z == 0) | ((z < 3) & (k < 2 * z - 1)))
        def _():
            gather_up(z, k, an.at[k]).start()

        @pl.when(z > 0)
        def _():
            gather_dn(z, k, an.at[k]).start()

    def start(k):
        @pl.when(k < NB)
        def _():
            norm(k)

        @pl.when(k > 0)
        def _():
            first_sends(k - 1)

    gain_copy.wait()
    @pl.when((z > 0) & (z < 3))
    def _():
        pl.semaphore_wait(barrier, 3)

    @pl.when((z == 0) | (z == 3))
    def _():
        pl.semaphore_wait(barrier, 2)

    loop(NB + 1, start)
    loop(2, lambda k: gather_pa(z, k, an.at[k]).start())
    rope_copy = pltpu.make_async_copy(rope_ref, rope, rope_m)
    rope_copy.start()
    for g in range(3):
        for copy in w_copies(g):
            copy.start()
    acc[...] = jnp.zeros_like(acc)

    def multiply(g, k, chunks):
        for c in chunks:
            got_pa(c, k)

        @pl.when(g + 3 < 3 * NB)
        def _():
            for copy in w_copies(g + 3):
                copy.start()

        for copy in w_copies(g):
            copy.wait()
        project(g, k, chunks, 0, 1)

    c0 = (3 - z) // 3

    def slot0(k):
        @pl.when(k < NB)
        def _():
            comm(0, k)

        @pl.when(k + 2 < NB)
        def _():
            gather_pa(z, k + 2, an.at[k + 2]).start()

        @pl.when(k > 0)
        def _():
            project(k - 1, k - 1, (z, c0), 1, 3)

        @pl.when(k < NB)
        def _():
            multiply(k, k, (z, c0))

    loop(NB + 1, slot0)

    def later_sends(s):
        @pl.when(z == s)
        def _():
            lax.fori_loop(2 * s - 1, NB, lambda k, _: gather_up(z, k, an.at[k]).start(), None)

    later_sends(1)
    wo_start(z != 1)
    rope_copy.wait()
    turn(0, z)
    turn(1, c0)
    freed(c0)

    pl.semaphore_signal(pcred.at[z], 1, device_id=partner, device_id_type=MESH)

    @pl.when(z < 3)
    def _():
        pl.semaphore_signal(ncred.at[z], 1, device_id=up, device_id_type=MESH)

    @pl.when(z > 0)
    def _():
        pl.semaphore_signal(ncred.at[z], 1, device_id=dn, device_id_type=MESH)

    outer = (z == 0) | (z == 3)
    firsts = (0, 2 - z // 2, 3 - z // 3, 4)
    attend(1 - z // 2)

    def own_sent():
        all_sent(z, pa_m)

        @pl.when(z > 0)
        def _():
            all_sent(z, dn_m)

        @pl.when(z < 3)
        def _():
            all_sent(z, up_m)

    two = (z % 3) // 2
    one = (z % 3) % 2
    for s in (1, 2):
        cp = (2 - z // 2, 3 - z // 3)[s - 1]
        cs = (1 - (z + 1) // 3, 2 - z // 2)[s - 1]
        lag = (LAGS[0] * two, LAGS[1] * one + LAGS[2] * two)[s - 1]
        summing = (z != 1) if s == 1 else (z >= 0)
        acc[0] = jnp.zeros_like(acc[0])

        def sums(j):
            @pl.when(summing)
            def _():
                @pl.when((j >= 0) & (j < NB))
                def _():
                    wo_next(j)

                if s == 1:
                    stages(j, 0, cs, False)
                else:
                    stages(j, 0, cs, z != 1)

                    @pl.when(z == 1)
                    def _():
                        stages(j, 1, 0, False)

        def slot(k):
            g = s * NB + k

            @pl.when(k < NB)
            def _():
                comm(s, k)

            sums(k - lag)

            @pl.when(k > 0)
            def _():
                project(g - 1, k - 1, (cp,), 1, 3)

            @pl.when(k < NB)
            def _():
                multiply(g, k, (cp,))

        loop(NB + 1, slot)
        wo_start(outer)
        if s == 1:
            later_sends(2)
        turn(0, cp)
        if s == 2:
            freed(cp)
        lax.fori_loop(firsts[s], firsts[s + 1], lambda c, _: attend(c), None)
        if s == 1:
            freed(cp)

            @pl.when(z == 1)
            def _():
                attend(0)

        loop(lag, lambda k: sums(NB + 1 + k - lag))
        wo_start(~outer)
        if s == 1:
            pl.when(z == 1)(own_sent)

    @pl.when(outer)
    def _():
        def last(j):
            @pl.when(j < NB)
            def _():
                wo_next(j)

            stages(j, 0, 3 - z // 3, z >= 0)

        loop(NB + 1, last)
        wo_start(outer)

        @pl.when(z == 0)
        def _():
            attend(0)


    def home(j):
        @pl.when(j < NB)
        def _():
            wo_next(j)

        @pl.when((z == 1) | (z == 2))
        def _():
            stages(j, 0, 3, z >= 0)

        stages(j, 1, z, None, 3)

    loop(NB + 3, home)

    pl.when(z != 1)(own_sent)
    loop(NB, lambda k: run_dn(0, 0, k).wait_send())

    @pl.when(z == 1)
    def _():
        remote(an, xg.at[0, :, pl.ds(0, RB), :], ns_m.at[NB], nb_r.at[0, 0], dn).wait_send()


def _fused(x, gain, wq, wk, wv, wo, rope):
    RB, D = x.shape
    HD = wq.shape[1]
    H, KB, C = HD // HEAD, D // NB, 2 * RB
    dma = pltpu.SemaphoreType.DMA
    return pl.pallas_call(
        _kernel,
        out_shape=pltpu.VMEM((RB, D), BF16),
        in_specs=[pl.BlockSpec(memory_space=pl.ANY)] * 7,
        out_specs=pl.BlockSpec(memory_space=pltpu.VMEM),
        scratch_shapes=[
            pltpu.VMEM((RB, D), BF16),
            pltpu.VMEM((NB, RB, KB), BF16),
            pltpu.VMEM((D,), BF16),
            pltpu.VMEM(rope.shape, F32),
            pltpu.VMEM((4, NB, C, KB), BF16),
            pltpu.VMEM((4, 3, KB, HD), BF16),
            pltpu.VMEM((3, HD, KB), BF16),
            pltpu.VMEM((2, C, 3 * HD), F32),
            pltpu.VMEM((4, C, HD), BF16),
            pltpu.VMEM((4, H, C, HEAD), BF16),
            pltpu.VMEM((4, H, HEAD, C), BF16),
            pltpu.VMEM((H, HEAD + 8, C), F32),
            pltpu.VMEM((H, C), F32),
            pltpu.VMEM((NB, RB, KB), BF16),
            pltpu.VMEM((6, C, KB), F32),
            pltpu.VMEM((6, RB, KB), BF16),
            pltpu.VMEM((NB, RB, KB), BF16),
            dma,
            dma,
            dma,
            dma((4, 3)),
            dma((3,)),
            dma((4,)),
            dma((4,)),
            dma((4,)),
            dma((4, NB)),
            dma((4, NB)),
            dma((6,)),
            dma((NB + 1,)),
            dma((NB,)),
            pltpu.SemaphoreType.REGULAR((4,)),
            pltpu.SemaphoreType.REGULAR((4,)),
        ],
        compiler_params=pltpu.CompilerParams(collective_id=0, has_side_effects=True, vmem_limit_bytes=67043328 - 2 * RB * D - 65536),
    )(x, gain, wq, wk, wv, wo, rope)


def _rope(rows):
    half = HEAD // 2
    angle = np.arange(rows, dtype=np.float32)[:, None] * np.float32(THETA) ** (-np.arange(half, dtype=np.float32) / np.float32(half))
    return np.concatenate([np.cos(angle), np.sin(angle)], 1).astype(np.float32)


def solution(mesh):
    def step(x, gain, wq, wk, wv, wo):
        return _fused(x, gain, wq, wk, wv, wo, jnp.asarray(_rope(x.shape[0] * mesh.shape["tp"])))

    tokens, columns = P(("dp", "tp"), None), P(None, "tp")
    return jax.shard_map(
        step,
        mesh=mesh,
        in_specs=(tokens, P(None), columns, columns, columns, P("tp", None)),
        out_specs=tokens,
        check_vma=False,
    )
```

```python
import jax
import jax.numpy as jnp
import numpy as np
from jax import lax
from jax.experimental import pallas as pl
from jax.experimental.pallas import tpu as pltpu
from jax.sharding import PartitionSpec as P

HEAD = 128
THETA = 10000
NB = 16
HIDDEN = -2e30
LOG2E = 1.4426950408889634
LAGS = (6, 4, 10)
MESH = pl.DeviceIdType.MESH
F32, BF16 = jnp.float32, jnp.bfloat16


def _dot(a, b, ca=1, cb=0):
    return lax.dot_general(a, b, (((ca,), (cb,)), ((), ())), preferred_element_type=F32)


def _kernel(x_ref, gain_ref, wq_ref, wk_ref, wv_ref, wo_ref, rope_ref, y_ref,
            xv, an, gain_v, rope, xg, wbuf, wob, acc, q_s, k_s, vt_s, mix_s, top_s, second, term, pst, nst,
            x_m, gain_m, rope_m, w_m, wo_m, up_m, dn_m, pa_m, nb_r, pa_r, tp_m, ns_m, sec_r, pcred, ncred):
    RB, D = x_ref.shape
    HD = wq_ref.shape[1]
    H = HD // HEAD
    KB = D // NB
    C = 2 * RB
    TN = HD
    me = lax.axis_index("tp")
    z, r = me // 2, me % 2
    up, dn, partner = {"tp": me + 2}, {"tp": me - 2}, {"tp": me + 1 - 2 * r}
    weights = (wq_ref, wk_ref, wv_ref)

    def remote(src, dst, send, recv, to):
        return pltpu.make_async_remote_copy(src_ref=src, dst_ref=dst, send_sem=send, recv_sem=recv, device_id=to, device_id_type=MESH)

    def half(c, k, h):
        return xg.at[c, k, pl.ds(pl.multiple_of(h * RB, RB), RB), :]

    def gather_up(c, k, src):
        return remote(src, half(c, k, r), up_m.at[c], nb_r.at[c, k], up)

    def gather_dn(c, k, src):
        return remote(src, half(c, k, r), dn_m.at[c], nb_r.at[c, k], dn)

    def gather_pa(c, k, src):
        return remote(src, half(c, k, r), pa_m.at[c], pa_r.at[c, k], partner)

    def all_sent(c, sem):
        remote(an, xg.at[c, :, pl.ds(0, RB), :], sem.at[c], nb_r.at[c, 0], partner).wait_send()

    def got_pa(c, k):
        remote(half(c, k, 1 - r), half(c, k, 1 - r), pa_m.at[c], pa_r.at[c, k], partner).wait_recv()

    def block(k):
        return pl.ds(pl.multiple_of(k * KB, KB), KB)

    def w_copies(g):
        at = pl.ds(pl.multiple_of((g % NB) * KB, KB), KB)
        return [pltpu.make_async_copy(weights[i].at[at, :], wbuf.at[g % 4, i], w_m.at[g % 4, i]) for i in range(3)]

    def wo_copy(j):
        return pltpu.make_async_copy(wo_ref.at[:, block(j)], wob.at[j % 3], wo_m.at[j % 3])

    def loop(n, body):
        lax.fori_loop(0, n, lambda i, _: body(i), None)

    def from_below(s, k, here):
        @pl.when(here)
        def _():
            gather_up(s, k, half(s, k, r)).wait_recv()

            @pl.when(z < 3)
            def _():
                gather_up(s, k, half(s, k, r)).start()

            gather_pa(s, k, half(s, k, r)).start()

    def comm(s, k):
        from_below(s, k, (z == 3) | ((z == 2) & (k > 0)) if s == 1 else z > s)
        d = z + 1 + s

        @pl.when(d <= 3)
        def _():
            gather_dn(d, k, half(d, k, r)).wait_recv()

            @pl.when(z > 0)
            def _():
                gather_dn(d, k, half(d, k, r)).start()

            gather_pa(d, k, half(d, k, r)).start()

    def freed(c):
        @pl.when((z > c) & (z < 3))
        def _():
            all_sent(c, up_m)

        @pl.when((z < c) & (z > 0))
        def _():
            all_sent(c, dn_m)

        all_sent(c, pa_m)
        pl.semaphore_signal(pcred.at[c], 1, device_id=partner, device_id_type=MESH)

        @pl.when((c <= z) & (z < 3))
        def _():
            pl.semaphore_signal(ncred.at[c], 1, device_id=up, device_id_type=MESH)

        @pl.when((c >= z) & (z > 0))
        def _():
            pl.semaphore_signal(ncred.at[c], 1, device_id=dn, device_id_type=MESH)

    def project(g, k, chunks, first, last):
        n = HD // TN

        def tile(t, _):
            i, at = t // n, pl.multiple_of((t % n) * TN, TN)
            w = wbuf[g % 4, i, :, pl.ds(at, TN)]
            cols = pl.ds(pl.multiple_of(t * TN, TN), TN)
            for p, c in enumerate(chunks):
                acc[p, :, cols] += _dot(xg[c, k], w)

        lax.fori_loop(first * n, last * n, tile, None)

    def turn(p, c):
        rows = pl.ds(pl.multiple_of(c * C, C), C)
        cs = rope[rows, :]
        sc = pltpu.roll(cs, HEAD // 2, 1)
        first = lax.broadcasted_iota(jnp.int32, cs.shape, 1) < HEAD // 2
        cos, sin = jnp.where(first, cs, sc), jnp.where(first, -sc, cs)

        def turned(t):
            t = t.astype(BF16).astype(F32)
            return (t * cos + pltpu.roll(t, HEAD // 2, 1) * sin).astype(BF16)

        for h in range(H):
            at = h * HEAD
            q_s[c, :, at : at + HEAD] = turned(acc[p, :, at : at + HEAD])
            k_s[c, h] = turned(acc[p, :, HD + at : HD + at + HEAD])
            vt_s[c, h] = acc[p, :, 2 * HD + at : 2 * HD + at + HEAD].astype(BF16).T

    def attend(c):
        e = HEAD**-0.5 * LOG2E
        ones = jnp.ones((8, C), BF16)

        def scores(kb):
            return [_dot(k_s[kb, h], q_s[c, :, h * HEAD : (h + 1) * HEAD], 1, 1) for h in range(H)]

        def values(kb, h):
            return jnp.concatenate([vt_s[kb, h], ones], axis=0)

        ok = lax.broadcasted_iota(jnp.int32, (C, C), 1) >= lax.broadcasted_iota(jnp.int32, (C, C), 0)
        for h, s in enumerate(scores(c)):
            s = jnp.where(ok, s, HIDDEN)
            top = s.max(axis=0, keepdims=True)
            top_s[h : h + 1, :] = top
            mix_s[h] = _dot(values(c, h), jnp.exp2((s - top) * e).astype(BF16))

        def block(kb, _):
            weights, keeps = [], []
            for h, s in enumerate(scores(kb)):
                old = top_s[h : h + 1, :]
                top = jnp.maximum(old, s.max(axis=0, keepdims=True))
                top_s[h : h + 1, :] = top
                weights.append(jnp.exp2((s - top) * e).astype(BF16))
                keeps.append(jnp.exp2((old - top) * e))
            for h in range(H):
                mix_s[h] = mix_s[h] * keeps[h] + _dot(values(kb, h), weights[h])

        lax.fori_loop(0, c, block, None)
        for h in range(H):
            out = mix_s[h, :HEAD, :] * (1 / mix_s[h, HEAD : HEAD + 1, :])
            q_s[c, :, h * HEAD : (h + 1) * HEAD] = out.T.astype(BF16)

    def slot_of(w, j):
        return 2 + j % 4 if w else j % 2

    def my_rows(w, j):
        return term.at[slot_of(w, j), pl.ds(pl.multiple_of(r * RB, RB), RB), :]

    def to_partner(w, c, j):
        return remote(pst.at[slot_of(w, j)], xg.at[c, j, pl.ds(RB, RB), :], tp_m.at[slot_of(w, j)], pa_r.at[c, j], partner)

    def staged(w):
        return an if w else nst

    def run_dn(w, c, j):
        return remote(staged(w).at[j], xg.at[c, j, pl.ds(0, RB), :], ns_m.at[w * NB + j * (1 - w)], nb_r.at[c, j], dn)

    def run_up(w, c, j):
        return remote(staged(w).at[j], xg.at[c, j, pl.ds(0, RB), :], ns_m.at[w * NB + j * (1 - w)], nb_r.at[c, j], up)

    def run_home(w, j):
        return remote(staged(w).at[j], second.at[j], ns_m.at[w * NB + j * (1 - w)], sec_r.at[j], up)

    def wo_start(when):
        @pl.when(when)
        def _():
            wo_copy(0).start()
            wo_copy(1).start()

    def wo_next(j):
        @pl.when(j + 2 < NB)
        def _():
            wo_copy(j + 2).start()

        wo_copy(j).wait()

    def stage_a(w, c, j):
        @pl.when(j == 0)
        def _():
            pl.semaphore_wait(pcred.at[c], 1)

        tk = min(512, KB)

        def tile(n):
            cols = pl.ds(pl.multiple_of(n * tk, tk), tk)
            term[slot_of(w, j), :, cols] = _dot(q_s[c], wob[j % 3, :, cols])

        loop(KB // tk, tile)
        theirs = pl.ds(pl.multiple_of((1 - r) * RB, RB), RB)
        pst[slot_of(w, j)] = term[slot_of(w, j), theirs, :].astype(BF16)
        to_partner(w, c, j).start()

    def stage_b(w, c, j, prior):
        to_partner(w, c, j).wait()
        t = my_rows(w, j)
        t[...] += xg[c, j, RB:, :].astype(F32)

        @pl.when(((c <= z) & (z < 3)) | ((c > z) & (z > 0)))
        def _():
            run_dn(w, c, j).wait_recv()
            t[...] += xg[c, j, :RB, :].astype(F32)

        if prior is None:
            @pl.when(z > 0)
            def _():
                run_home(w, j).wait_recv()
                t[...] += second[j].astype(F32)

            y_ref[:, block(j)] = (xv[:, block(j)].astype(F32) + t[...]).astype(BF16)
            return

        if prior is not False:
            @pl.when(prior)
            def _():
                run_dn(w, c, j).wait_send()

        @pl.when(j == 0)
        def _():
            pl.semaphore_wait(ncred.at[c], 1)

        staged(w)[j] = t[...].astype(BF16)

        @pl.when(c < z)
        def _():
            run_dn(w, c, j).start()

        @pl.when(c == z + 1)
        def _():
            run_home(w, j).start()

        @pl.when(c > z + 1)
        def _():
            run_up(w, c, j).start()

    def stages(j, w, c, prior, late=1):
        @pl.when((j >= 0) & (j < NB))
        def _():
            stage_a(w, c, j)

        @pl.when((j >= late) & (j < NB + late))
        def _():
            stage_b(w, c, j - late, prior)

    loop(NB, lambda k: pltpu.make_async_copy(x_ref.at[:, block(k)], xv.at[:, block(k)], x_m).start())
    gain_copy = pltpu.make_async_copy(gain_ref, gain_v, gain_m)
    gain_copy.start()
    barrier = pltpu.get_barrier_semaphore()
    pl.semaphore_signal(barrier, 1, device_id=partner, device_id_type=MESH)

    @pl.when(z > 0)
    def _():
        pl.semaphore_signal(barrier, 1, device_id=dn, device_id_type=MESH)

    @pl.when(z < 3)
    def _():
        pl.semaphore_signal(barrier, 1, device_id=up, device_id_type=MESH)

    def squares(k, total):
        t = xv[:, block(k)].astype(F32)
        t = t * t
        for i in range(0, KB, 128):
            total = total + t[:, i : i + 128]
        return total

    pltpu.make_async_copy(x_ref, xv, x_m).wait()
    total = lax.fori_loop(0, NB, squares, jnp.zeros((RB, 128), F32))
    scale = lax.rsqrt(jnp.sum(total, axis=1, keepdims=True) * (1 / D) + 1e-6)

    def norm(k):
        gain = gain_v[block(k)].astype(F32).reshape(1, KB)
        t = (xv[:, block(k)].astype(F32) * scale * gain).astype(BF16)
        an[k] = t
        xg[z, k, pl.ds(pl.multiple_of(r * RB, RB), RB), :] = t

    def first_sends(k):
        @pl.when((z == 0) | ((z < 3) & (k < z)))
        def _():
            gather_up(z, k, an.at[k]).start()

        @pl.when(z > 0)
        def _():
            gather_dn(z, k, an.at[k]).start()

    def start(k):
        @pl.when(k < NB)
        def _():
            norm(k)

        @pl.when(k > 0)
        def _():
            first_sends(k - 1)

    gain_copy.wait()
    @pl.when((z > 0) & (z < 3))
    def _():
        pl.semaphore_wait(barrier, 3)

    @pl.when((z == 0) | (z == 3))
    def _():
        pl.semaphore_wait(barrier, 2)

    loop(NB + 1, start)
    loop(2, lambda k: gather_pa(z, k, an.at[k]).start())
    rope_copy = pltpu.make_async_copy(rope_ref, rope, rope_m)
    rope_copy.start()
    for g in range(3):
        for copy in w_copies(g):
            copy.start()
    acc[...] = jnp.zeros_like(acc)

    def multiply(g, k, chunks):
        for c in chunks:
            got_pa(c, k)

        @pl.when(g + 3 < 3 * NB)
        def _():
            for copy in w_copies(g + 3):
                copy.start()

        for copy in w_copies(g):
            copy.wait()
        project(g, k, chunks, 0, 1)

    c0 = (3 - z) // 3

    def later_sends(s):
        @pl.when(z == s)
        def _():
            lax.fori_loop(s, NB, lambda k, _: gather_up(z, k, an.at[k]).start(), None)

    def slot0(k):
        @pl.when(k < NB)
        def _():
            comm(0, k)

        @pl.when(k == NB - 1)
        def _():
            later_sends(1)
            from_below(1, 0, z == 2)

        @pl.when(k + 2 < NB)
        def _():
            gather_pa(z, k + 2, an.at[k + 2]).start()

        @pl.when(k > 0)
        def _():
            project(k - 1, k - 1, (z, c0), 1, 3)

        @pl.when(k < NB)
        def _():
            multiply(k, k, (z, c0))

    loop(NB + 1, slot0)

    wo_start(z != 1)
    rope_copy.wait()
    turn(0, z)
    turn(1, c0)
    freed(c0)

    pl.semaphore_signal(pcred.at[z], 1, device_id=partner, device_id_type=MESH)

    @pl.when(z < 3)
    def _():
        pl.semaphore_signal(ncred.at[z], 1, device_id=up, device_id_type=MESH)

    @pl.when(z > 0)
    def _():
        pl.semaphore_signal(ncred.at[z], 1, device_id=dn, device_id_type=MESH)

    outer = (z == 0) | (z == 3)
    firsts = (0, 2 - z // 2, 3 - z // 3, 4)
    attend(1 - z // 2)

    def own_sent():
        all_sent(z, pa_m)

        @pl.when(z > 0)
        def _():
            all_sent(z, dn_m)

        @pl.when(z < 3)
        def _():
            all_sent(z, up_m)

    two = (z % 3) // 2
    one = (z % 3) % 2
    for s in (1, 2):
        cp = (2 - z // 2, 3 - z // 3)[s - 1]
        cs = (1 - (z + 1) // 3, 2 - z // 2)[s - 1]
        lag = (LAGS[0] * two, LAGS[1] * one + LAGS[2] * two)[s - 1]
        summing = (z != 1) if s == 1 else (z >= 0)
        acc[0] = jnp.zeros_like(acc[0])

        def sums(j):
            @pl.when(summing)
            def _():
                @pl.when((j >= 0) & (j < NB))
                def _():
                    wo_next(j)

                if s == 1:
                    stages(j, 0, cs, False)
                else:
                    stages(j, 0, cs, z != 1)

                    @pl.when(z == 1)
                    def _():
                        stages(j, 1, 0, False)

        def slot(k):
            g = s * NB + k

            @pl.when(k < NB)
            def _():
                comm(s, k)

            sums(k - lag)

            @pl.when(k > 0)
            def _():
                project(g - 1, k - 1, (cp,), 1, 3)

            @pl.when(k < NB)
            def _():
                multiply(g, k, (cp,))

        loop(NB + 1, slot)
        wo_start(outer)
        if s == 1:
            later_sends(2)
        turn(0, cp)
        if s == 2:
            freed(cp)
        lax.fori_loop(firsts[s], firsts[s + 1], lambda c, _: attend(c), None)
        if s == 1:
            freed(cp)

            @pl.when(z == 1)
            def _():
                attend(0)

        loop(lag, lambda k: sums(NB + 1 + k - lag))
        wo_start(~outer)
        if s == 1:
            pl.when(z == 1)(own_sent)

    @pl.when(outer)
    def _():
        def last(j):
            @pl.when(j < NB)
            def _():
                wo_next(j)

            stages(j, 0, 3 - z // 3, z >= 0)

        loop(NB + 1, last)
        wo_start(outer)

        @pl.when(z == 0)
        def _():
            attend(0)


    def home(j):
        @pl.when(j < NB)
        def _():
            wo_next(j)

        @pl.when((z == 1) | (z == 2))
        def _():
            stages(j, 0, 3, z >= 0)

        stages(j, 1, z, None, 3)

    loop(NB + 3, home)

    pl.when(z != 1)(own_sent)
    loop(NB, lambda k: run_dn(0, 0, k).wait_send())

    @pl.when(z == 1)
    def _():
        remote(an, xg.at[0, :, pl.ds(0, RB), :], ns_m.at[NB], nb_r.at[0, 0], dn).wait_send()


def _fused(x, gain, wq, wk, wv, wo, rope):
    RB, D = x.shape
    HD = wq.shape[1]
    H, KB, C = HD // HEAD, D // NB, 2 * RB
    dma = pltpu.SemaphoreType.DMA
    return pl.pallas_call(
        _kernel,
        out_shape=pltpu.VMEM((RB, D), BF16),
        in_specs=[pl.BlockSpec(memory_space=pl.ANY)] * 7,
        out_specs=pl.BlockSpec(memory_space=pltpu.VMEM),
        scratch_shapes=[
            pltpu.VMEM((RB, D), BF16),
            pltpu.VMEM((NB, RB, KB), BF16),
            pltpu.VMEM((D,), BF16),
            pltpu.VMEM(rope.shape, F32),
            pltpu.VMEM((4, NB, C, KB), BF16),
            pltpu.VMEM((4, 3, KB, HD), BF16),
            pltpu.VMEM((3, HD, KB), BF16),
            pltpu.VMEM((2, C, 3 * HD), F32),
            pltpu.VMEM((4, C, HD), BF16),
            pltpu.VMEM((4, H, C, HEAD), BF16),
            pltpu.VMEM((4, H, HEAD, C), BF16),
            pltpu.VMEM((H, HEAD + 8, C), F32),
            pltpu.VMEM((H, C), F32),
            pltpu.VMEM((NB, RB, KB), BF16),
            pltpu.VMEM((6, C, KB), F32),
            pltpu.VMEM((6, RB, KB), BF16),
            pltpu.VMEM((NB, RB, KB), BF16),
            dma,
            dma,
            dma,
            dma((4, 3)),
            dma((3,)),
            dma((4,)),
            dma((4,)),
            dma((4,)),
            dma((4, NB)),
            dma((4, NB)),
            dma((6,)),
            dma((NB + 1,)),
            dma((NB,)),
            pltpu.SemaphoreType.REGULAR((4,)),
            pltpu.SemaphoreType.REGULAR((4,)),
        ],
        compiler_params=pltpu.CompilerParams(collective_id=0, has_side_effects=True, vmem_limit_bytes=67043328 - 2 * RB * D - 65536),
    )(x, gain, wq, wk, wv, wo, rope)


def _rope(rows):
    half = HEAD // 2
    angle = np.arange(rows, dtype=np.float32)[:, None] * np.float32(THETA) ** (-np.arange(half, dtype=np.float32) / np.float32(half))
    return np.concatenate([np.cos(angle), np.sin(angle)], 1).astype(np.float32)


def solution(mesh):
    def step(x, gain, wq, wk, wv, wo):
        return _fused(x, gain, wq, wk, wv, wo, jnp.asarray(_rope(x.shape[0] * mesh.shape["tp"])))

    tokens, columns = P(("dp", "tp"), None), P(None, "tp")
    return jax.shard_map(
        step,
        mesh=mesh,
        in_specs=(tokens, P(None), columns, columns, columns, P("tp", None)),
        out_specs=tokens,
        check_vma=False,
    )
```
